8 devices in a mesh: seqs: 1 (over z), states: 8 (over y, x, core).
Axes of the slice: x: 2, y: 2, z: 1, core: 2. Of those that a mesh axis runs over, the one named last changes fastest.
Arguments:
- trans_mat: bfloat16 [16384, 16384], P(None, 'states')
- emit_mat: bfloat16 [16384, 10000], P('states')
- init_prob: float32 [16384], P('states')
- tokens: int32 [128, 64], P('seqs')
- lengths: int32 [128], P('seqs')
Outputs:
- output 1: float32 [128], P('seqs')
- output 2: float32 [128, 16384], P('seqs', 'states')
All inputs are finite; a program needn't handle non-finite values.
Results may differ from the reference program's by a relative error of at most 0.001.
Values are sent between devices in bfloat16 or wider.
A program may use at most 1 GiB of HBM per device.

```python
import jax
import jax.numpy as jnp
from jax import lax

STATES = 16384
VOCAB = 10000
SEQS = 128
STEPS = 64


def draw_lengths(len_key):
    k_len, k_full, k_short = jax.random.split(len_key, 3)
    lengths = jax.random.randint(k_len, (SEQS,), 1, STEPS + 1, jnp.int32)
    full_row = jax.random.randint(k_full, (), 0, SEQS, jnp.int32)
    short_row = (full_row + 1 + jax.random.randint(k_short, (), 0, SEQS - 1, jnp.int32)) % SEQS
    row_ids = jnp.arange(SEQS, dtype=jnp.int32)
    lengths = jnp.where(row_ids == full_row, STEPS, lengths)
    lengths = jnp.where(row_ids == short_row, 1, lengths)
    return lengths


def setup_inputs(seed: int = 0, part: int = 0) -> dict:
    root_key = jax.random.key(seed)
    k_trans, k_emit, k_init, k_part = jax.random.split(root_key, 4)
    k_part = jax.random.fold_in(k_part, part)
    k_tok, k_len = jax.random.split(k_part, 2)
    trans_mat = jax.nn.softmax(1.5 * jax.random.normal(k_trans, (STATES, STATES), jnp.float32), axis=1).astype(jnp.bfloat16)
    emit_mat = jax.nn.softmax(2.5 * jax.random.normal(k_emit, (STATES, VOCAB), jnp.float32), axis=1).astype(jnp.bfloat16)
    init_prob = jax.nn.softmax(1.5 * jax.random.normal(k_init, (STATES,), jnp.float32))
    tokens = jax.random.randint(k_tok, (SEQS, STEPS), 0, VOCAB, jnp.int32)
    lengths = draw_lengths(k_len)
    return {"trans_mat": trans_mat, "emit_mat": emit_mat, "init_prob": init_prob, "tokens": tokens, "lengths": lengths}


def reference(trans_mat, emit_mat, init_prob, tokens, lengths):
    first_emit = jnp.take(emit_mat, tokens[:, 0], axis=1).T.astype(jnp.float32)
    first_prob = init_prob[None, :] * first_emit
    first_norm = jnp.sum(first_prob, axis=1)
    state_prob = first_prob / first_norm[:, None]
    log_lik = jnp.log(first_norm)

    def one_step(carried, inputs):
        state_prob, log_lik = carried
        token_col, step_idx = inputs
        predicted = jnp.dot(state_prob.astype(jnp.bfloat16), trans_mat, preferred_element_type=jnp.float32)
        new_prob = predicted * jnp.take(emit_mat, token_col, axis=1).T.astype(jnp.float32)
        step_norm = jnp.sum(new_prob, axis=1)
        new_prob = new_prob / step_norm[:, None]
        is_live = step_idx < lengths
        state_prob = jnp.where(is_live[:, None], new_prob, state_prob)
        log_lik = log_lik + jnp.where(is_live, jnp.log(step_norm), 0.0)
        return (state_prob, log_lik), None

    step_ids = jnp.arange(1, tokens.shape[1], dtype=jnp.int32)
    (state_prob, log_lik), _ = lax.scan(one_step, (state_prob, log_lik), (tokens[:, 1:].T, step_ids))
    return (log_lik, state_prob)
```

```python
import functools

import jax
import jax.numpy as jnp
from jax import lax
from jax.experimental import pallas as pl
from jax.experimental.pallas import tpu as pltpu
from jax.sharding import PartitionSpec as P

N_DEV = 8
SEQS = 128
OWN = 2048
PIECE = 512
WIDE = 256
STEPS = 63
BF16 = jnp.bfloat16
F32 = jnp.float32


def place(g, k):
    late = g // 6
    mid = (g + 6) // 8 - late
    r = g % 2 + mid * (2 + 2 * (k % 2)) + late * 6
    j = mid * (k // 2 + 2 * (g // 4)) + (1 - mid) * k
    return r, j


def step_kernel(m, steps, depth, t0_ref, a_hbm, e_hbm, st_in, len_row, len_col, ll_in, st_out, ll_out,
                fixed, ring, gath, e_buf, st, acc, part, sums, recip,
                fixed_sem, ring_sem, e_sem, st_sem, recv_sem, own_sem, fwd_sem, c_send, c_recv):
    me = lax.axis_index("states")
    core = me % 2
    xx = (me // 2) % 2
    yy = me // 4

    def dev(r):
        return me + (r % 2) * (1 - 2 * core) + ((r // 2) % 2) * (2 - 4 * xx) + (r // 4) * (4 - 8 * yy)

    def remote(src, dst, send, recv, r):
        return pltpu.make_async_remote_copy(
            src_ref=src, dst_ref=dst, send_sem=send, recv_sem=recv,
            device_id={"states": dev(r)}, device_id_type=pl.DeviceIdType.MESH,
        )

    def rows_of(g, k):
        r, j = place(g, k)
        return a_hbm.at[pl.ds(pl.multiple_of(dev(r) * OWN + j * PIECE, PIECE), PIECE)]

    def ring_copy(g):
        return pltpu.make_async_copy(rows_of(g, 3), ring.at[g % depth], ring_sem.at[g % depth])

    def start_fixed(g):
        for k in range(3):
            pltpu.make_async_copy(rows_of(g, k), fixed.at[3 * g + k], fixed_sem.at[g]).start()

    def wait_fixed(g):
        pltpu.make_async_copy(fixed.at[pl.ds(3 * g, 3)], fixed.at[pl.ds(3 * g, 3)], fixed_sem.at[g]).wait()

    def send_piece(slot, j):
        src = gath.at[slot, j]
        x_pos = 8 + 8 * (j // 2) + 2 * (j % 2)
        for r, pos in ((2, x_pos), (4, x_pos + 1), (1, 4 + j)):
            remote(src, gath.at[slot, pos], own_sem.at[slot], recv_sem.at[slot, pos], r).start()

    def received(slot, pos):
        pltpu.make_async_copy(gath.at[slot, pos], gath.at[slot, pos], recv_sem.at[slot, pos]).wait()

    def forward(slot, pos, to, r):
        remote(gath.at[slot, pos], gath.at[slot, to], fwd_sem.at[slot], recv_sem.at[slot, to], r).start()

    def product(slot, g, n):
        cols = slice(n * WIDE, (n + 1) * WIDE)
        got = jnp.dot(gath[slot, 4 * g], fixed[3 * g, :, cols], preferred_element_type=F32)
        for k in range(1, 4):
            rows = fixed[3 * g + k, :, cols] if k < 3 else ring[g % depth, :, cols]
            got = got + jnp.dot(gath[slot, 4 * g + k], rows, preferred_element_type=F32)
        return got

    def begin_group(s, g):
        ring_copy((g + depth - 1) % 8).start()

        @pl.when(s == 0)
        def _():
            wait_fixed(g)

            @pl.when(g + 2 < 8)
            def _():
                start_fixed(g + 2)

        ring_copy(g).wait()

    st_copy = pltpu.make_async_copy(st_in.at[pl.ds(0, m)], st, st_sem.at[0])
    st_copy.start()
    ring_copy(0).start()
    start_fixed(0)
    for g in range(1, depth - 1):
        ring_copy(g).start()
    start_fixed(1)
    pltpu.make_async_copy(e_hbm.at[0], e_buf, e_sem.at[0]).start()

    barrier = pltpu.get_barrier_semaphore()
    for r in range(1, N_DEV):
        pl.semaphore_signal(barrier, inc=1, device_id={"states": dev(r)}, device_id_type=pl.DeviceIdType.MESH)

    ll_out[...] = ll_in[...]
    if m < SEQS:
        sums[...] = jnp.zeros_like(sums)
    t0 = t0_ref[0]
    lens_row = len_row[...]

    st_copy.wait()
    pl.semaphore_wait(barrier, N_DEV - 1)
    for j in range(4):
        gath[0, j] = st[:, j * PIECE:(j + 1) * PIECE].astype(BF16)
        if j:
            send_piece(0, j - 1)
    send_piece(0, 3)

    def one_step(s, carry):
        slot = s % 2
        then = 1 - slot

        begin_group(s, 0)
        for n in range(8):
            acc[n] = product(slot, 0, n)

        def group(g, carry):
            for k in range(4):
                pos = 4 * g + k
                received(slot, pos)
                if k % 2 == 0:
                    @pl.when(g == 2)
                    def _():
                        forward(slot, pos, 24 + k // 2, 4)
                else:
                    @pl.when(g == 4)
                    def _():
                        forward(slot, pos, 26 + k // 2, 2)

                @pl.when(g % 2 == 0)
                def _():
                    forward(slot, pos, pos + 4, 1)

            begin_group(s, g)
            for n in range(8):
                acc[n] += product(slot, g, n)
            return carry

        lax.fori_loop(1, 7, group, 0)

        for k in range(4):
            received(slot, 28 + k)
        begin_group(s, 7)
        pltpu.make_async_copy(e_hbm.at[s], e_buf, e_sem.at[0]).wait()
        both = jnp.zeros((m, 128), F32)
        for n in range(8):
            a = (acc[n] + product(slot, 7, n)) * e_buf[:, n * WIDE:(n + 1) * WIDE].astype(F32)
            acc[n] = a
            both = both + (a[:, :128] + a[:, 128:])
        sums[:m] = both

        part[slot, me] = jnp.sum(sums[...].T.reshape(16, 8, 128), axis=0)
        for r in range(1, N_DEV):
            remote(part.at[slot, me], part.at[slot, me], c_send.at[slot], c_recv.at[slot], r).start()

        @pl.when(s + 1 < steps)
        def _():
            pltpu.make_async_copy(e_hbm.at[s + 1], e_buf, e_sem.at[0]).start()

        pltpu.make_async_copy(gath.at[slot, pl.ds(0, 12)], gath.at[slot, pl.ds(0, 12)], own_sem.at[slot]).wait()
        pltpu.make_async_copy(gath.at[slot, pl.ds(0, 16)], gath.at[slot, pl.ds(0, 16)], fwd_sem.at[slot]).wait()
        pltpu.make_async_copy(part.at[slot, pl.ds(0, 7)], part.at[slot, pl.ds(0, 7)], c_recv.at[slot]).wait()
        whole = part[slot, 0]
        for d in range(1, N_DEV):
            whole = whole + part[slot, d]
        norm = jnp.sum(whole, axis=0, keepdims=True)
        recip[...] = jnp.broadcast_to(1.0 / norm, (128, 128)).T
        t = t0 + s
        ll_out[...] = ll_out[...] + jnp.where(t < lens_row, jnp.log(norm), 0.0)
        pltpu.make_async_copy(part.at[slot, pl.ds(0, 7)], part.at[slot, pl.ds(0, 7)], c_send.at[slot]).wait()

        scale = recip[:m]
        live = t < len_col[:m]
        for j in range(4):
            for q in range(4):
                at = j * PIECE + q * 128
                cols = slice(at, at + 128)
                new = jnp.where(live, acc[at // WIDE, :, (q % 2) * 128:(q % 2 + 1) * 128] * scale, st[:, cols])
                st[:, cols] = new
                gath[then, j, :, q * 128:(q + 1) * 128] = new.astype(BF16)
            if j:
                @pl.when(s + 1 < steps)
                def _():
                    send_piece(then, j - 1)

        @pl.when(s + 1 < steps)
        def _():
            send_piece(then, 3)

        return carry

    lax.fori_loop(0, steps, one_step, 0)

    for g in range(depth - 1):
        ring_copy(g).wait()
    out_copy = pltpu.make_async_copy(st, st_out.at[pl.ds(0, m)], st_sem.at[0])
    out_copy.start()
    out_copy.wait()


def run_steps(m, steps, t0, trans, emis, state, len_row, len_col, log_lik):
    vmem = pl.BlockSpec(memory_space=pltpu.VMEM)
    hbm = pl.BlockSpec(memory_space=pl.ANY)
    depth = 2 if m > 80 else 4
    dma = pltpu.SemaphoreType.DMA
    return pl.pallas_call(
        functools.partial(step_kernel, m, steps, depth),
        out_shape=(jax.ShapeDtypeStruct((SEQS, OWN), F32), jax.ShapeDtypeStruct((1, SEQS), F32)),
        in_specs=[pl.BlockSpec(memory_space=pltpu.SMEM), hbm, hbm, hbm, vmem, vmem, vmem],
        out_specs=(hbm, vmem),
        scratch_shapes=[
            pltpu.VMEM((24, PIECE, OWN), BF16),
            pltpu.VMEM((depth, PIECE, OWN), BF16),
            pltpu.VMEM((2, 32, m, PIECE), BF16),
            pltpu.VMEM((m, OWN), BF16),
            pltpu.VMEM((m, OWN), F32),
            pltpu.VMEM((8, m, WIDE), F32),
            pltpu.VMEM((2, N_DEV, 8, 128), F32),
            pltpu.VMEM((128, 128), F32),
            pltpu.VMEM((128, 128), F32),
            dma((8,)), dma((depth,)), dma((1,)), dma((1,)), dma((2, 32)), dma((2,)), dma((2,)), dma((2,)), dma((2,)),
        ],
        input_output_aliases={3: 0},
        compiler_params=pltpu.CompilerParams(
            collective_id=0, has_side_effects=True, vmem_limit_bytes=67043328
        ),
        name=f"steps_{m}",
    )(t0, trans, emis, state, len_row, len_col, log_lik)


def solution(mesh):
    def local_run(trans_cols, emit_rows, init_part, token_rows, length_rows):
        emit_t = emit_rows.T
        first_prob = init_part[None, :] * jnp.take(emit_t, token_rows[:, 0], axis=0, mode="clip").astype(F32)
        first_norm = lax.psum(jnp.sum(first_prob, axis=1), "states")
        state = first_prob / first_norm[:, None]
        log_lik = jnp.log(first_norm)[None, :]
        tokens = token_rows[:, 1:].T.reshape(-1)
        emis = jnp.take(emit_t, tokens, axis=0, mode="clip").reshape(STEPS, SEQS, OWN)
        len_row = length_rows[None, :]
        len_col = jnp.broadcast_to(length_rows[:, None], (SEQS, 128))
        t0 = jnp.ones((1,), jnp.int32)
        state, log_lik = run_steps(SEQS, STEPS, t0, trans_cols, emis, state, len_row, len_col, log_lik)
        return log_lik[0], state

    return jax.shard_map(
        local_run,
        mesh=mesh,
        in_specs=(P(None, "states"), P("states", None), P("states"), P("seqs", None), P("seqs")),
        out_specs=(P("seqs"), P("seqs", "states")),
        check_vma=False,
    )
```

```python
import functools

import jax
import jax.numpy as jnp
from jax import lax
from jax.experimental import pallas as pl
from jax.experimental.pallas import tpu as pltpu
from jax.sharding import PartitionSpec as P

N_DEV = 8
SEQS = 128
OWN = 2048
PIECE = 512
WIDE = 256
STEPS = 63
SEGMENT = 9
ROWS = (48, 64, 80, 96, 112, 128)
BF16 = jnp.bfloat16
F32 = jnp.float32


def place(g, k):
    late = g // 6
    mid = (g + 6) // 8 - late
    r = g % 2 + mid * (2 + 2 * (k % 2)) + late * 6
    j = mid * (k // 2 + 2 * (g // 4)) + (1 - mid) * k
    return r, j


def distances(me):
    core = me % 2
    xx = (me // 2) % 2
    yy = me // 4

    def dev(r):
        return me + (r % 2) * (1 - 2 * core) + ((r // 2) % 2) * (2 - 4 * xx) + (r // 4) * (4 - 8 * yy)

    return dev


def remote_copy(dev, src, dst, send, recv, r):
    return pltpu.make_async_remote_copy(
        src_ref=src, dst_ref=dst, send_sem=send, recv_sem=recv,
        device_id={"states": dev(r)}, device_id_type=pl.DeviceIdType.MESH,
    )


def signal_all(dev):
    barrier = pltpu.get_barrier_semaphore()
    for r in range(1, N_DEV):
        pl.semaphore_signal(barrier, inc=1, device_id={"states": dev(r)}, device_id_type=pl.DeviceIdType.MESH)
    return barrier


def send_sums(me, dev, sums, part, send, recv):
    part[me] = jnp.sum(sums[...].T.reshape(16, 8, 128), axis=0)
    for r in range(1, N_DEV):
        remote_copy(dev, part.at[me], part.at[me], send, recv, r).start()


def add_sums(part, recv):
    pltpu.make_async_copy(part.at[pl.ds(0, 7)], part.at[pl.ds(0, 7)], recv).wait()
    whole = part[0]
    for d in range(1, N_DEV):
        whole = whole + part[d]
    return jnp.sum(whole, axis=0, keepdims=True)


def first_kernel(raw, alpha, ll, part, sums, send, recv):
    me = lax.axis_index("states")
    dev = distances(me)
    barrier = signal_all(dev)
    both = jnp.zeros((SEQS, 128), F32)
    for q in range(16):
        both = both + raw[:, q * 128:(q + 1) * 128]
    sums[...] = both
    pl.semaphore_wait(barrier, N_DEV - 1)
    send_sums(me, dev, sums, part, send, recv)
    norm = add_sums(part, recv)
    ll[...] = jnp.log(norm)
    scale = jnp.broadcast_to(1.0 / norm, (128, 128)).T
    for q in range(16):
        alpha[:, q * 128:(q + 1) * 128] = raw[:, q * 128:(q + 1) * 128] * scale
    pltpu.make_async_copy(part.at[pl.ds(0, 7)], part.at[pl.ds(0, 7)], send).wait()


def run_first(number, raw):
    vmem = pl.BlockSpec(memory_space=pltpu.VMEM)
    return pl.pallas_call(
        first_kernel,
        out_shape=(jax.ShapeDtypeStruct((SEQS, OWN), F32), jax.ShapeDtypeStruct((1, SEQS), F32)),
        in_specs=[vmem],
        out_specs=(vmem, vmem),
        scratch_shapes=[
            pltpu.VMEM((N_DEV, 8, 128), F32),
            pltpu.VMEM((128, 128), F32),
            pltpu.SemaphoreType.DMA,
            pltpu.SemaphoreType.DMA,
        ],
        compiler_params=pltpu.CompilerParams(collective_id=number, has_side_effects=True, vmem_limit_bytes=8 << 20),
        name="first",
    )(raw)


def step_kernel(m, steps, depth, t0_ref, a_hbm, e_hbm, st_in, len_row, len_col, ll_in, st_out, ll_out,
                fixed, ring, gath, e_buf, st, acc, part, sums, recip,
                fixed_sem, ring_sem, e_sem, st_sem, recv_sem, own_sem, fwd_sem, c_send, c_recv):
    me = lax.axis_index("states")
    dev = distances(me)

    def remote(src, dst, send, recv, r):
        return remote_copy(dev, src, dst, send, recv, r)

    def rows_of(g, k):
        r, j = place(g, k)
        return a_hbm.at[pl.ds(pl.multiple_of(dev(r) * OWN + j * PIECE, PIECE), PIECE)]

    def ring_copy(g):
        return pltpu.make_async_copy(rows_of(g, 3), ring.at[g % depth], ring_sem.at[g % depth])

    def start_fixed(g):
        for k in range(3):
            pltpu.make_async_copy(rows_of(g, k), fixed.at[3 * g + k], fixed_sem.at[g]).start()

    def wait_fixed(g):
        pltpu.make_async_copy(fixed.at[pl.ds(3 * g, 3)], fixed.at[pl.ds(3 * g, 3)], fixed_sem.at[g]).wait()

    def send_piece(slot, j):
        src = gath.at[slot, j]
        x_pos = 8 + 8 * (j // 2) + 2 * (j % 2)
        for r, pos in ((2, x_pos), (4, x_pos + 1), (1, 4 + j)):
            remote(src, gath.at[slot, pos], own_sem.at[slot], recv_sem.at[slot, pos], r).start()

    def received(slot, pos):
        pltpu.make_async_copy(gath.at[slot, pos], gath.at[slot, pos], recv_sem.at[slot, pos]).wait()

    def forward(slot, pos, to, r):
        remote(gath.at[slot, pos], gath.at[slot, to], fwd_sem.at[slot], recv_sem.at[slot, to], r).start()

    def product(slot, g, n):
        cols = slice(n * WIDE, (n + 1) * WIDE)
        got = jnp.dot(gath[slot, 4 * g], fixed[3 * g, :, cols], preferred_element_type=F32)
        for k in range(1, 4):
            rows = fixed[3 * g + k, :, cols] if k < 3 else ring[g % depth, :, cols]
            got = got + jnp.dot(gath[slot, 4 * g + k], rows, preferred_element_type=F32)
        return got

    def begin_group(s, g):
        ring_copy((g + depth - 1) % 8).start()

        @pl.when(s == 0)
        def _():
            wait_fixed(g)

            @pl.when(g + 2 < 8)
            def _():
                start_fixed(g + 2)

        ring_copy(g).wait()

    st_copy = pltpu.make_async_copy(st_in.at[pl.ds(0, m)], st, st_sem.at[0])
    st_copy.start()
    ring_copy(0).start()
    start_fixed(0)
    for g in range(1, depth - 1):
        ring_copy(g).start()
    start_fixed(1)
    pltpu.make_async_copy(e_hbm.at[0], e_buf, e_sem.at[0]).start()

    barrier = signal_all(dev)
    if m < SEQS:
        sums[...] = jnp.zeros_like(sums)
    t0 = t0_ref[0]
    lens_row = len_row[...]

    def total(slot):
        send_sums(me, dev, sums, part.at[slot], c_send.at[slot], c_recv.at[slot])

    def total_done(slot):
        norm = add_sums(part.at[slot], c_recv.at[slot])
        recip[...] = jnp.broadcast_to(1.0 / norm, (128, 128)).T
        return norm

    def total_sent(slot):
        pltpu.make_async_copy(part.at[slot, pl.ds(0, 7)], part.at[slot, pl.ds(0, 7)], c_send.at[slot]).wait()

    ll_out[...] = ll_in[...]
    st_copy.wait()
    pl.semaphore_wait(barrier, N_DEV - 1)
    for j in range(4):
        gath[0, j] = st[:, j * PIECE:(j + 1) * PIECE].astype(BF16)
        if j:
            send_piece(0, j - 1)
    send_piece(0, 3)

    def one_step(s, carry):
        slot = s % 2
        then = 1 - slot

        def group(g, carry):
            for k in range(4):
                pos = 4 * g + k

                @pl.when(g >= 1)
                def _():
                    received(slot, pos)

                if k % 2 == 0:
                    @pl.when(g == 2)
                    def _():
                        forward(slot, pos, 24 + k // 2, 4)
                else:
                    @pl.when(g == 4)
                    def _():
                        forward(slot, pos, 26 + k // 2, 2)

                @pl.when((1 - g % 2) * g > 0)
                def _():
                    forward(slot, pos, pos + 4, 1)

            begin_group(s, g)
            for n in range(8):
                acc[n] = jnp.where(g > 0, acc[n], 0.0) + product(slot, g, n)
            return carry

        lax.fori_loop(0, 7, group, 0)

        for k in range(4):
            received(slot, 28 + k)
        begin_group(s, 7)
        pltpu.make_async_copy(e_hbm.at[s], e_buf, e_sem.at[0]).wait()
        both = jnp.zeros((m, 128), F32)
        for n in range(8):
            a = (acc[n] + product(slot, 7, n)) * e_buf[:, n * WIDE:(n + 1) * WIDE].astype(F32)
            acc[n] = a
            both = both + (a[:, :128] + a[:, 128:])
        sums[:m] = both

        total(slot)

        @pl.when(s + 1 < steps)
        def _():
            pltpu.make_async_copy(e_hbm.at[s + 1], e_buf, e_sem.at[0]).start()

        pltpu.make_async_copy(gath.at[slot, pl.ds(0, 12)], gath.at[slot, pl.ds(0, 12)], own_sem.at[slot]).wait()
        pltpu.make_async_copy(gath.at[slot, pl.ds(0, 16)], gath.at[slot, pl.ds(0, 16)], fwd_sem.at[slot]).wait()
        norm = total_done(slot)
        t = t0 + s
        ll_out[...] = ll_out[...] + jnp.where(t < lens_row, jnp.log(norm), 0.0)
        total_sent(slot)

        scale = recip[:m]
        live = t < len_col[:m]
        for j in range(4):
            for q in range(4):
                at = j * PIECE + q * 128
                cols = slice(at, at + 128)
                new = jnp.where(live, acc[at // WIDE, :, (q % 2) * 128:(q % 2 + 1) * 128] * scale, st[:, cols])
                st[:, cols] = new
                gath[then, j, :, q * 128:(q + 1) * 128] = new.astype(BF16)
            if j:
                @pl.when(s + 1 < steps)
                def _():
                    send_piece(then, j - 1)

        @pl.when(s + 1 < steps)
        def _():
            send_piece(then, 3)

        return carry

    lax.fori_loop(0, steps, one_step, 0)

    for g in range(depth - 1):
        ring_copy(g).wait()
    out_copy = pltpu.make_async_copy(st, st_out.at[pl.ds(0, m)], st_sem.at[0])
    out_copy.start()
    out_copy.wait()


def run_steps(m, steps, number, t0, trans, emis, state, len_row, len_col, log_lik):
    vmem = pl.BlockSpec(memory_space=pltpu.VMEM)
    hbm = pl.BlockSpec(memory_space=pl.ANY)
    depth = 2 if m > 80 else 4
    dma = pltpu.SemaphoreType.DMA
    return pl.pallas_call(
        functools.partial(step_kernel, m, steps, depth),
        out_shape=(jax.ShapeDtypeStruct((SEQS, OWN), F32), jax.ShapeDtypeStruct((1, SEQS), F32)),
        in_specs=[pl.BlockSpec(memory_space=pltpu.SMEM), hbm, hbm, hbm, vmem, vmem, vmem],
        out_specs=(hbm, vmem),
        scratch_shapes=[
            pltpu.VMEM((24, PIECE, OWN), BF16),
            pltpu.VMEM((depth, PIECE, OWN), BF16),
            pltpu.VMEM((2, 32, m, PIECE), BF16),
            pltpu.VMEM((m, OWN), BF16),
            pltpu.VMEM((m, OWN), F32),
            pltpu.VMEM((8, m, WIDE), F32),
            pltpu.VMEM((2, N_DEV, 8, 128), F32),
            pltpu.VMEM((128, 128), F32),
            pltpu.VMEM((128, 128), F32),
            dma((8,)), dma((depth,)), dma((1,)), dma((1,)), dma((2, 32)), dma((2,)), dma((2,)), dma((2,)), dma((2,)),
        ],
        input_output_aliases={3: 0},
        compiler_params=pltpu.CompilerParams(
            collective_id=number, has_side_effects=True, vmem_limit_bytes=67043328
        ),
        name=f"steps_{m}_{number}",
    )(t0, trans, emis, state, len_row, len_col, log_lik)


def solution(mesh):
    def local_run(trans_cols, emit_rows, init_part, token_rows, length_rows):
        emit_t = emit_rows.T

        def emissions(tokens):
            return jnp.take(emit_t, tokens.reshape(-1), axis=0, mode="clip").reshape(*tokens.shape, OWN)

        key = length_rows * SEQS + (SEQS - 1 - jnp.arange(SEQS, dtype=jnp.int32))
        rank = jnp.sum((key[None, :] > key[:, None]).astype(jnp.int32), axis=1)
        pick = (rank[None, :] == jnp.arange(SEQS, dtype=jnp.int32)[:, None]).astype(jnp.int32)
        lens = jnp.sum(pick * length_rows[None, :], axis=1)
        tokens = jnp.sum(token_rows.T[:, None, :] * pick[None], axis=2)
        len_row = lens[None, :]
        len_col = jnp.broadcast_to(lens[:, None], (SEQS, 128))

        def segment(m, number, t0, state, log_lik):
            part = lax.dynamic_slice_in_dim(tokens, t0, SEGMENT, axis=0)[:, :m]
            return run_steps(m, SEGMENT, number, jnp.reshape(t0, (1,)), trans_cols, emissions(part), state,
                             len_row, len_col, log_lik)

        state, log_lik = run_first(0, init_part[None, :] * emissions(tokens[0]).astype(F32))

        def later(seg, carried):
            t0 = 1 + SEGMENT * seg
            live = jnp.sum((lens > t0).astype(jnp.int32))
            which = sum((live > m).astype(jnp.int32) for m in ROWS[:-1])
            branches = [functools.partial(segment, m, 1 + i) for i, m in enumerate(ROWS)]
            return lax.switch(which, branches, t0, *carried)

        state, log_lik = lax.fori_loop(0, STEPS // SEGMENT, later, (state, log_lik))
        return jnp.take(log_lik[0], rank, mode="clip"), jnp.take(state, rank, axis=0, mode="clip")

    return jax.shard_map(
        local_run,
        mesh=mesh,
        in_specs=(P(None, "states"), P("states", None), P("states"), P("seqs", None), P("seqs")),
        out_specs=(P("seqs"), P("seqs", "states")),
        check_vma=False,
    )
```

```python
import functools

import jax
import jax.numpy as jnp
from jax import lax
from jax.experimental import pallas as pl
from jax.experimental.pallas import tpu as pltpu
from jax.sharding import PartitionSpec as P

N_DEV = 8
SEQS = 128
OWN = 2048
PIECE = 512
WIDE = 256
STEPS = 63
SEGMENT = 9
ROWS = (32, 48, 64, 80, 96, 112, 128)
BF16 = jnp.bfloat16
F32 = jnp.float32


def place(g, k):
    late = g // 6
    mid = (g + 6) // 8 - late
    low = 1 - mid - late
    odd = k % 2
    direct = 1 - k // 2
    r = low * g + mid * (2 + 2 * odd + direct) + late * (7 - direct)
    j = low * k + mid * ((g - 2 + 2 * odd) % 4) + late * (g - 6 + 2 * odd)
    return r, j


def distances(me):
    core = me % 2
    xx = (me // 2) % 2
    yy = me // 4

    def dev(r):
        return me + (r % 2) * (1 - 2 * core) + ((r // 2) % 2) * (2 - 4 * xx) + (r // 4) * (4 - 8 * yy)

    return dev


def remote_copy(dev, src, dst, send, recv, r):
    return pltpu.make_async_remote_copy(
        src_ref=src, dst_ref=dst, send_sem=send, recv_sem=recv,
        device_id={"states": dev(r)}, device_id_type=pl.DeviceIdType.MESH,
    )


def signal_all(dev):
    barrier = pltpu.get_barrier_semaphore()
    for r in range(1, N_DEV):
        pl.semaphore_signal(barrier, inc=1, device_id={"states": dev(r)}, device_id_type=pl.DeviceIdType.MESH)
    return barrier


def send_sums(me, dev, sums, part, send, recv):
    part[me] = jnp.sum(sums[...].T.reshape(16, 8, 128), axis=0)
    for r in range(N_DEV - 1, 0, -1):
        remote_copy(dev, part.at[me], part.at[me], send, recv, r).start()


def add_sums(part, recv):
    pltpu.make_async_copy(part.at[pl.ds(0, 7)], part.at[pl.ds(0, 7)], recv).wait()
    whole = part[0]
    for d in range(1, N_DEV):
        whole = whole + part[d]
    return jnp.sum(whole, axis=0, keepdims=True)


def first_kernel(raw, alpha, ll, part, sums, send, recv):
    me = lax.axis_index("states")
    dev = distances(me)
    barrier = signal_all(dev)
    both = jnp.zeros((SEQS, 128), F32)
    for q in range(16):
        both = both + raw[:, q * 128:(q + 1) * 128]
    sums[...] = both
    pl.semaphore_wait(barrier, N_DEV - 1)
    send_sums(me, dev, sums, part, send, recv)
    norm = add_sums(part, recv)
    ll[...] = jnp.log(norm)
    scale = jnp.broadcast_to(1.0 / norm, (128, 128)).T
    for q in range(16):
        alpha[:, q * 128:(q + 1) * 128] = raw[:, q * 128:(q + 1) * 128] * scale
    pltpu.make_async_copy(part.at[pl.ds(0, 7)], part.at[pl.ds(0, 7)], send).wait()


def run_first(number, raw):
    vmem = pl.BlockSpec(memory_space=pltpu.VMEM)
    return pl.pallas_call(
        first_kernel,
        out_shape=(jax.ShapeDtypeStruct((SEQS, OWN), F32), jax.ShapeDtypeStruct((1, SEQS), F32)),
        in_specs=[vmem],
        out_specs=(vmem, vmem),
        scratch_shapes=[
            pltpu.VMEM((N_DEV, 8, 128), F32),
            pltpu.VMEM((128, 128), F32),
            pltpu.SemaphoreType.DMA,
            pltpu.SemaphoreType.DMA,
        ],
        compiler_params=pltpu.CompilerParams(collective_id=number, has_side_effects=True, vmem_limit_bytes=8 << 20),
        name="first",
    )(raw)


def step_kernel(m, steps, depth, t0_ref, a_hbm, e_hbm, st_in, len_row, ll_in, st_out, ll_out,
                fixed, ring, gath, e_buf, st, acc, part, sums, recip, len_col,
                fixed_sem, ring_sem, e_sem, st_sem, recv_sem, own_sem, fwd_sem, c_send, c_recv):
    me = lax.axis_index("states")
    dev = distances(me)

    def remote(src, dst, send, recv, r):
        return remote_copy(dev, src, dst, send, recv, r)

    def rows_of(g, k):
        r, j = place(g, k)
        return a_hbm.at[pl.ds(pl.multiple_of(dev(r) * OWN + j * PIECE, PIECE), PIECE)]

    def ring_copy(g):
        return pltpu.make_async_copy(rows_of(g, 3), ring.at[g % depth], ring_sem.at[g % depth])

    def start_fixed(g):
        for k in range(3):
            pltpu.make_async_copy(rows_of(g, k), fixed.at[3 * g + k], fixed_sem.at[g]).start()

    def wait_fixed(g):
        pltpu.make_async_copy(fixed.at[pl.ds(3 * g, 3)], fixed.at[pl.ds(3 * g, 3)], fixed_sem.at[g]).wait()

    def send_piece(slot, j, r, pos):
        remote(gath.at[slot, j], gath.at[slot, pos], own_sem.at[slot], recv_sem.at[slot, pos], r).start()

    def send_pair(slot, j):
        send_piece(slot, j, 3, 8 + 4 * j)
        send_piece(slot, j + 2, 5, 9 + 4 * j)
        send_piece(slot, j, 1, 4 + j)
        send_piece(slot, j + 2, 1, 6 + j)

    def send_rest(slot):
        for j in range(2):
            send_piece(slot, j + 2, 3, 16 + 4 * j)
            send_piece(slot, j, 5, 17 + 4 * j)

    def received(slot, pos):
        pltpu.make_async_copy(gath.at[slot, pos], gath.at[slot, pos], recv_sem.at[slot, pos]).wait()

    def forward(slot, pos, to, r):
        remote(gath.at[slot, pos], gath.at[slot, to], fwd_sem.at[slot], recv_sem.at[slot, to], r).start()

    def arrived(slot, g, relay):
        for k in range(2):
            pos = 4 * g + k
            received(slot, pos)

            @pl.when(relay)
            def _():
                forward(slot, pos, pos + 16, 5 - 2 * k)

            forward(slot, pos, pos + 2, 1)

    def product(slot, g, b, n):
        cols = slice(n * WIDE, (n + 1) * WIDE)
        got = None
        for k in range(2 * b, 2 * b + 2):
            rows = fixed[3 * g + k, :, cols] if k < 3 else ring[g % depth, :, cols]
            one = jnp.dot(gath[slot, 4 * g + k], rows, preferred_element_type=F32)
            got = one if got is None else got + one
        return got

    def begin_group(s, g):
        ring_copy((g + depth - 1) % 8).start()

        @pl.when(s == 0)
        def _():
            wait_fixed(g)

            @pl.when(g + 2 < 8)
            def _():
                start_fixed(g + 2)

    st_copy = pltpu.make_async_copy(st_in.at[pl.ds(0, m)], st, st_sem.at[0])
    st_copy.start()
    ring_copy(0).start()
    start_fixed(0)
    for g in range(1, depth - 1):
        ring_copy(g).start()
    start_fixed(1)
    pltpu.make_async_copy(e_hbm.at[0], e_buf, e_sem.at[0]).start()

    barrier = signal_all(dev)
    if m < SEQS:
        sums[...] = jnp.zeros_like(sums)
    t0 = t0_ref[0]
    lens_row = len_row[...]
    len_col[...] = jnp.broadcast_to(lens_row.astype(F32), (128, 128)).T

    def total(slot):
        send_sums(me, dev, sums, part.at[slot], c_send.at[slot], c_recv.at[slot])

    def total_done(slot):
        norm = add_sums(part.at[slot], c_recv.at[slot])
        recip[...] = jnp.broadcast_to(1.0 / norm, (128, 128)).T
        return norm

    def total_sent(slot):
        pltpu.make_async_copy(part.at[slot, pl.ds(0, 7)], part.at[slot, pl.ds(0, 7)], c_send.at[slot]).wait()

    ll_out[...] = ll_in[...]
    st_copy.wait()
    pl.semaphore_wait(barrier, N_DEV - 1)
    for j in range(2):
        for i in (j, j + 2):
            gath[0, i] = st[:, i * PIECE:(i + 1) * PIECE].astype(BF16)
        send_pair(0, j)
    send_rest(0)

    def one_step(s, carry):
        slot = s % 2
        then = 1 - slot

        def group(g, carry):
            @pl.when(g == 1)
            def _():
                received(slot, 4)
                received(slot, 5)

            @pl.when(g == 2)
            def _():
                arrived(slot, 2, True)

            begin_group(s, g)
            for n in range(8):
                acc[n] = jnp.where(g > 0, acc[n], 0.0) + product(slot, g, 0, n)

            @pl.when(g >= 2)
            def _():
                arrived(slot, g + 1, g == 2)

            @pl.when(g >= 1)
            def _():
                received(slot, 4 * g + 2)
                received(slot, 4 * g + 3)

            ring_copy(g).wait()
            for n in range(8):
                acc[n] += product(slot, g, 1, n)
            return carry

        lax.fori_loop(0, 7, group, 0)

        begin_group(s, 7)
        for n in range(8):
            acc[n] += product(slot, 7, 0, n)
        received(slot, 30)
        received(slot, 31)
        ring_copy(7).wait()
        pltpu.make_async_copy(e_hbm.at[s], e_buf, e_sem.at[0]).wait()
        both = jnp.zeros((m, 128), F32)
        for n in range(8):
            a = (acc[n] + product(slot, 7, 1, n)) * e_buf[:, n * WIDE:(n + 1) * WIDE].astype(F32)
            acc[n] = a
            both = both + (a[:, :128] + a[:, 128:])
        sums[:m] = both

        total(slot)

        @pl.when(s + 1 < steps)
        def _():
            pltpu.make_async_copy(e_hbm.at[s + 1], e_buf, e_sem.at[0]).start()

        pltpu.make_async_copy(gath.at[slot, pl.ds(0, 12)], gath.at[slot, pl.ds(0, 12)], own_sem.at[slot]).wait()
        pltpu.make_async_copy(gath.at[slot, pl.ds(0, 16)], gath.at[slot, pl.ds(0, 16)], fwd_sem.at[slot]).wait()
        norm = total_done(slot)
        t = t0 + s
        ll_out[...] = ll_out[...] + jnp.where(t < lens_row, jnp.log(norm), 0.0)
        total_sent(slot)

        scale = recip[:m]
        live = t.astype(F32) < len_col[:m]
        for j in range(2):
            for i in (j, j + 2):
                for q in range(4):
                    at = i * PIECE + q * 128
                    cols = slice(at, at + 128)
                    new = jnp.where(live, acc[at // WIDE, :, (q % 2) * 128:(q % 2 + 1) * 128] * scale, st[:, cols])
                    st[:, cols] = new
                    gath[then, i, :, q * 128:(q + 1) * 128] = new.astype(BF16)

            @pl.when(s + 1 < steps)
            def _():
                send_pair(then, j)

        @pl.when(s + 1 < steps)
        def _():
            send_rest(then)

        return carry

    lax.fori_loop(0, steps, one_step, 0)

    for g in range(depth - 1):
        ring_copy(g).wait()
    out_copy = pltpu.make_async_copy(st, st_out.at[pl.ds(0, m)], st_sem.at[0])
    out_copy.start()
    out_copy.wait()


def pick_kernel(size, ahead, tokens, mods, emit, out, blocks, sem):
    i = pl.program_id(0)
    slots = ahead + 1

    def start(g):
        for q in range(size):
            row = pl.multiple_of((tokens[g * size + q] // 8) * 8, 8)
            pltpu.make_async_copy(
                emit.at[pl.ds(row, 8)], blocks.at[g % slots, pl.ds(8 * q, 8)], sem.at[g % slots]
            ).start()

    @pl.when(i == 0)
    def _():
        def some(g, carry):
            start(g)
            return carry

        lax.fori_loop(0, ahead, some, 0)

    @pl.when(i + ahead < pl.num_programs(0))
    def _():
        start(i + ahead)

    slot = i % slots
    pltpu.make_async_copy(blocks.at[slot], blocks.at[slot], sem.at[slot]).wait()
    row = lax.broadcasted_iota(jnp.int32, (size, 8 * size), 0)
    col = lax.broadcasted_iota(jnp.int32, (size, 8 * size), 1)
    want = row * 8 + jnp.concatenate([mods[...]] * (8 * size // 128), axis=1)
    ones = (col == want).astype(F32).astype(BF16)
    out[...] = jnp.dot(ones, blocks[slot], preferred_element_type=F32).astype(BF16)


def pick_rows(emit, tokens):
    (count,) = tokens.shape
    size = 48 if count % 48 == 0 else 32
    ahead = min(3, count // size)
    mods = jnp.broadcast_to((tokens % 8)[:, None], (count, 128))
    return pl.pallas_call(
        functools.partial(pick_kernel, size, ahead),
        out_shape=jax.ShapeDtypeStruct((count, OWN), BF16),
        grid_spec=pltpu.PrefetchScalarGridSpec(
            num_scalar_prefetch=1,
            grid=(count // size,),
            in_specs=[pl.BlockSpec((size, 128), lambda i, tok: (i, 0)), pl.BlockSpec(memory_space=pl.ANY)],
            out_specs=pl.BlockSpec((size, OWN), lambda i, tok: (i, 0)),
            scratch_shapes=[pltpu.VMEM((ahead + 1, 8 * size, OWN), BF16), pltpu.SemaphoreType.DMA((ahead + 1,))],
        ),
        compiler_params=pltpu.CompilerParams(vmem_limit_bytes=16 << 20),
        name="pick",
    )(tokens, mods, emit)


def run_steps(m, steps, number, t0, trans, emis, state, len_row, log_lik):
    vmem = pl.BlockSpec(memory_space=pltpu.VMEM)
    hbm = pl.BlockSpec(memory_space=pl.ANY)
    depth = 2 if m > 80 else 4
    dma = pltpu.SemaphoreType.DMA
    return pl.pallas_call(
        functools.partial(step_kernel, m, steps, depth),
        out_shape=(jax.ShapeDtypeStruct((SEQS, OWN), F32), jax.ShapeDtypeStruct((1, SEQS), F32)),
        in_specs=[pl.BlockSpec(memory_space=pltpu.SMEM), hbm, hbm, hbm, vmem, vmem],
        out_specs=(hbm, vmem),
        scratch_shapes=[
            pltpu.VMEM((24, PIECE, OWN), BF16),
            pltpu.VMEM((depth, PIECE, OWN), BF16),
            pltpu.VMEM((2, 32, m, PIECE), BF16),
            pltpu.VMEM((m, OWN), BF16),
            pltpu.VMEM((m, OWN), F32),
            pltpu.VMEM((8, m, WIDE), F32),
            pltpu.VMEM((2, N_DEV, 8, 128), F32),
            pltpu.VMEM((128, 128), F32),
            pltpu.VMEM((128, 128), F32),
            pltpu.VMEM((128, 128), F32),
            dma((8,)), dma((depth,)), dma((1,)), dma((1,)), dma((2, 32)), dma((2,)), dma((2,)), dma((2,)), dma((2,)),
        ],
        input_output_aliases={3: 0},
        compiler_params=pltpu.CompilerParams(
            collective_id=number, has_side_effects=True, vmem_limit_bytes=67043328
        ),
        name=f"steps_{m}_{number}",
    )(t0, trans, emis, state, len_row, log_lik)


def solution(mesh):
    def local_run(trans_cols, emit_rows, init_part, token_rows, length_rows):
        emit_t = emit_rows.T

        def emissions(tokens):
            return pick_rows(emit_t, tokens.reshape(-1)).reshape(*tokens.shape, OWN)

        key = length_rows * SEQS + (SEQS - 1 - jnp.arange(SEQS, dtype=jnp.int32))
        rank = jnp.sum((key[None, :] > key[:, None]).astype(jnp.int32), axis=1)
        pick = (rank[None, :] == jnp.arange(SEQS, dtype=jnp.int32)[:, None]).astype(jnp.int32)
        lens = jnp.sum(pick * length_rows[None, :], axis=1)
        tokens = jnp.sum(token_rows.T[:, None, :] * pick[None], axis=2)
        len_row = lens[None, :]

        def segment(m, number, t0, state, log_lik):
            part = lax.dynamic_slice_in_dim(tokens, t0, SEGMENT, axis=0)[:, :m]
            return run_steps(m, SEGMENT, number, jnp.reshape(t0, (1,)), trans_cols, emissions(part), state,
                             len_row, log_lik)

        state, log_lik = run_first(0, init_part[None, :] * emissions(tokens[0]).astype(F32))

        starts = 1 + SEGMENT * jnp.arange(STEPS // SEGMENT, dtype=jnp.int32)
        live = jnp.sum((lens[None, :] > starts[:, None]).astype(jnp.int32), axis=1)
        which = sum((live > m).astype(jnp.int32) for m in ROWS[:-1])

        def later(carried, seg):
            t0, kernel = seg
            branches = [functools.partial(segment, m, 1 + i) for i, m in enumerate(ROWS)]
            return lax.switch(kernel, branches, t0, *carried), None

        (state, log_lik), _ = lax.scan(later, (state, log_lik), (starts, which))
        return jnp.take(log_lik[0], rank, mode="clip"), jnp.take(state, rank, axis=0, mode="clip")

    return jax.shard_map(
        local_run,
        mesh=mesh,
        in_specs=(P(None, "states"), P("states", None), P("states"), P("seqs", None), P("seqs")),
        out_specs=(P("seqs"), P("seqs", "states")),
        check_vma=False,
    )
```

```python
import functools

import jax
import jax.numpy as jnp
from jax import lax
from jax.experimental import pallas as pl
from jax.experimental.pallas import tpu as pltpu
from jax.sharding import PartitionSpec as P

N_DEV = 8
SEQS = 128
OWN = 2048
PIECE = 512
WIDE = 256
STEPS = 63
SEGMENT = 9
ROWS = (32, 48, 64, 80, 96, 112, 128)
BF16 = jnp.bfloat16
F32 = jnp.float32


def place(g, k):
    late = g // 6
    mid = (g + 6) // 8 - late
    low = 1 - mid - late
    odd = k % 2
    direct = 1 - k // 2
    r = low * g + mid * (2 + 2 * odd + direct) + late * (7 - direct)
    j = low * k + mid * ((g - 2 + 2 * odd) % 4) + late * (g - 6 + 2 * odd)
    return r, j


def distances(me):
    core = me % 2
    xx = (me // 2) % 2
    yy = me // 4

    def dev(r):
        return me + (r % 2) * (1 - 2 * core) + ((r // 2) % 2) * (2 - 4 * xx) + (r // 4) * (4 - 8 * yy)

    return dev


def remote_copy(dev, src, dst, send, recv, r):
    return pltpu.make_async_remote_copy(
        src_ref=src, dst_ref=dst, send_sem=send, recv_sem=recv,
        device_id={"states": dev(r)}, device_id_type=pl.DeviceIdType.MESH,
    )


def signal_all(dev):
    barrier = pltpu.get_barrier_semaphore()
    for r in range(1, N_DEV):
        pl.semaphore_signal(barrier, inc=1, device_id={"states": dev(r)}, device_id_type=pl.DeviceIdType.MESH)
    return barrier


def send_sums(me, dev, sums, part, send, recv):
    part[me] = jnp.sum(sums[...].T, axis=0, keepdims=True)
    for r in range(N_DEV - 1, 0, -1):
        remote_copy(dev, part.at[me], part.at[me], send, recv, r).start()


def add_sums(part, recv):
    pltpu.make_async_copy(part.at[pl.ds(0, 7)], part.at[pl.ds(0, 7)], recv).wait()
    whole = part[0]
    for d in range(1, N_DEV):
        whole = whole + part[d]
    return whole


def first_kernel(raw, alpha, ll, part, sums, send, recv):
    me = lax.axis_index("states")
    dev = distances(me)
    barrier = signal_all(dev)
    both = jnp.zeros((SEQS, 128), F32)
    for q in range(16):
        both = both + raw[:, q * 128:(q + 1) * 128]
    sums[...] = both
    pl.semaphore_wait(barrier, N_DEV - 1)
    send_sums(me, dev, sums, part, send, recv)
    norm = add_sums(part, recv)
    ll[...] = jnp.log(norm)
    scale = jnp.broadcast_to(1.0 / norm, (128, 128)).T
    for q in range(16):
        alpha[:, q * 128:(q + 1) * 128] = raw[:, q * 128:(q + 1) * 128] * scale
    pltpu.make_async_copy(part.at[pl.ds(0, 7)], part.at[pl.ds(0, 7)], send).wait()


def run_first(number, raw):
    vmem = pl.BlockSpec(memory_space=pltpu.VMEM)
    return pl.pallas_call(
        first_kernel,
        out_shape=(jax.ShapeDtypeStruct((SEQS, OWN), F32), jax.ShapeDtypeStruct((1, SEQS), F32)),
        in_specs=[vmem],
        out_specs=(vmem, vmem),
        scratch_shapes=[
            pltpu.VMEM((N_DEV, 1, 128), F32),
            pltpu.VMEM((128, 128), F32),
            pltpu.SemaphoreType.DMA,
            pltpu.SemaphoreType.DMA,
        ],
        compiler_params=pltpu.CompilerParams(collective_id=number, has_side_effects=True, vmem_limit_bytes=8 << 20),
        name="first",
    )(raw)


def step_kernel(m, steps, depth, t0_ref, a_hbm, e_hbm, st_in, len_row, ll_in, st_out, ll_out,
                fixed, ring, gath, e_buf, st, acc, part, sums, recip, len_col,
                fixed_sem, ring_sem, e_sem, st_sem, recv_sem, own_sem, fwd_sem, c_send, c_recv):
    me = lax.axis_index("states")
    dev = distances(me)

    def remote(src, dst, send, recv, r):
        return remote_copy(dev, src, dst, send, recv, r)

    def rows_of(pos):
        r, j = place(pos // 4, pos % 4)
        return a_hbm.at[pl.ds(pl.multiple_of(dev(r) * OWN + j * PIECE, PIECE), PIECE)]

    def begins(b):
        return 4 * b + 2 * ((b + 6) // 8)

    def ring_copy(b):
        return pltpu.make_async_copy(rows_of(begins(b) + 1), ring.at[b % depth], ring_sem.at[b % depth])

    def start_fixed(b, positions):
        for k, pos in enumerate(positions):
            pltpu.make_async_copy(rows_of(pos), fixed.at[3 * b + k], fixed_sem.at[b]).start()

    def start_block(b):
        start_fixed(b, [begins(b), begins(b) + 2, begins(b) + 3])

    def wait_fixed(b):
        pltpu.make_async_copy(fixed.at[pl.ds(3 * b, 3)], fixed.at[pl.ds(3 * b, 3)], fixed_sem.at[b]).wait()

    def send_piece(slot, j, r, pos):
        remote(gath.at[slot, j], gath.at[slot, pos], own_sem.at[slot], recv_sem.at[slot, pos], r).start()

    def send_pair(slot, j):
        send_piece(slot, j, 3, 8 + 4 * j)
        send_piece(slot, j + 2, 5, 9 + 4 * j)
        send_piece(slot, j, 1, 4 + j)
        send_piece(slot, j + 2, 1, 6 + j)

    def send_rest(slot):
        for j in range(2):
            send_piece(slot, j + 2, 3, 16 + 4 * j)
            send_piece(slot, j, 5, 17 + 4 * j)

    def received(slot, pos):
        pltpu.make_async_copy(gath.at[slot, pos], gath.at[slot, pos], recv_sem.at[slot, pos]).wait()

    def forward(slot, pos, to, r):
        remote(gath.at[slot, pos], gath.at[slot, to], fwd_sem.at[slot], recv_sem.at[slot, to], r).start()

    def arrived(slot, g, relay):
        for k in range(2):
            pos = 4 * g + k
            received(slot, pos)

            @pl.when(relay)
            def _():
                forward(slot, pos, pos + 16, 5 - 2 * k)

            forward(slot, pos, pos + 2, 1)

    def product(parts, n):
        cols = slice(n * WIDE, (n + 1) * WIDE)
        got = None
        for left, right in parts:
            one = jnp.dot(left[...], right[:, cols], preferred_element_type=F32)
            got = one if got is None else got + one
        return got

    def next_ring(b):
        ring_copy((b + depth - 1) % 8).start()

    st_copy = pltpu.make_async_copy(st_in.at[pl.ds(0, m)], st, st_sem.at[0])
    st_copy.start()
    ring_copy(0).start()
    start_block(0)
    for b in range(1, depth - 1):
        ring_copy(b).start()
    start_block(1)
    pltpu.make_async_copy(e_hbm.at[0], e_buf, e_sem.at[0]).start()

    barrier = signal_all(dev)
    if m < SEQS:
        sums[...] = jnp.zeros_like(sums)
    t0 = t0_ref[0]
    lens_row = len_row[...]
    len_col[...] = jnp.broadcast_to(lens_row.astype(F32), (128, 128)).T

    def total(slot):
        send_sums(me, dev, sums, part.at[slot], c_send.at[slot], c_recv.at[slot])

    def total_done(slot):
        norm = add_sums(part.at[slot], c_recv.at[slot])
        recip[...] = jnp.broadcast_to(1.0 / norm, (128, 128)).T
        return norm

    def total_sent(slot):
        pltpu.make_async_copy(part.at[slot, pl.ds(0, 7)], part.at[slot, pl.ds(0, 7)], c_send.at[slot]).wait()

    ll_out[...] = ll_in[...]
    st_copy.wait()
    pl.semaphore_wait(barrier, N_DEV - 1)
    for j in range(2):
        for i in (j, j + 2):
            gath[0, i] = st[:, i * PIECE:(i + 1) * PIECE].astype(BF16)
        send_pair(0, j)
    send_rest(0)

    def one_step(s, carry):
        slot = s % 2
        then = 1 - slot

        def block(b, carry):
            @pl.when(b == 1)
            def _():
                for k in range(4):
                    received(slot, 4 + k)

            @pl.when(b == 2)
            def _():
                arrived(slot, 2, True)

                @pl.when(s == 0)
                def _():
                    wait_fixed(7)
                    start_block(3)

                for n in range(8):
                    acc[n] += product([(gath.at[slot, 8], fixed.at[21]), (gath.at[slot, 9], fixed.at[22])], n)

            @pl.when(b >= 2)
            def _():
                arrived(slot, b + 1, b == 2)
                received(slot, 4 * b + 2)
                received(slot, 4 * b + 3)

            next_ring(b)

            @pl.when(s == 0)
            def _():
                wait_fixed(b)

                @pl.when(b == 0)
                def _():
                    start_fixed(7, [8, 9, 30])

                @pl.when(b == 1)
                def _():
                    start_block(2)

                @pl.when((b - 1) * (5 - b) > 0)
                def _():
                    start_block(b + 2)

            ring_copy(b).wait()
            left = [gath.at[slot, begins(b) + k] for k in range(4)]
            right = [fixed.at[3 * b], ring.at[b % depth], fixed.at[3 * b + 1], fixed.at[3 * b + 2]]
            for n in range(8):
                acc[n] = jnp.where(b > 0, acc[n], 0.0) + product(list(zip(left, right)), n)
            return carry

        lax.fori_loop(0, 7, block, 0)

        received(slot, 30)
        received(slot, 31)
        next_ring(7)
        ring_copy(7).wait()
        parts = [(gath.at[slot, 30], fixed.at[23]), (gath.at[slot, 31], ring.at[7 % depth])]
        pltpu.make_async_copy(e_hbm.at[s], e_buf, e_sem.at[0]).wait()
        both = jnp.zeros((m, 128), F32)
        for n in range(8):
            a = (acc[n] + product(parts, n)) * e_buf[:, n * WIDE:(n + 1) * WIDE].astype(F32)
            acc[n] = a
            both = both + (a[:, :128] + a[:, 128:])
        sums[:m] = both

        total(slot)

        @pl.when(s + 1 < steps)
        def _():
            pltpu.make_async_copy(e_hbm.at[s + 1], e_buf, e_sem.at[0]).start()

        pltpu.make_async_copy(gath.at[slot, pl.ds(0, 12)], gath.at[slot, pl.ds(0, 12)], own_sem.at[slot]).wait()
        pltpu.make_async_copy(gath.at[slot, pl.ds(0, 16)], gath.at[slot, pl.ds(0, 16)], fwd_sem.at[slot]).wait()
        norm = total_done(slot)
        t = t0 + s
        ll_out[...] = ll_out[...] + jnp.where(t < lens_row, jnp.log(norm), 0.0)
        total_sent(slot)

        scale = recip[:m]
        live = t.astype(F32) < len_col[:m]
        for j in range(2):
            for i in (j, j + 2):
                for q in range(4):
                    at = i * PIECE + q * 128
                    cols = slice(at, at + 128)
                    new = jnp.where(live, acc[at // WIDE, :, (q % 2) * 128:(q % 2 + 1) * 128] * scale, st[:, cols])
                    st[:, cols] = new
                    gath[then, i, :, q * 128:(q + 1) * 128] = new.astype(BF16)

            @pl.when(s + 1 < steps)
            def _():
                send_pair(then, j)

        @pl.when(s + 1 < steps)
        def _():
            send_rest(then)

        return carry

    lax.fori_loop(0, steps, one_step, 0)

    for b in range(depth - 1):
        ring_copy(b).wait()
    out_copy = pltpu.make_async_copy(st, st_out.at[pl.ds(0, m)], st_sem.at[0])
    out_copy.start()
    out_copy.wait()


def pick_kernel(size, ahead, rows, mods, emit, out, blocks, sem):
    i = pl.program_id(0)
    slots = ahead + 1

    def start(g):
        for q in range(size):
            row = pl.multiple_of(rows[g * size + q], 8)
            pltpu.make_async_copy(
                emit.at[pl.ds(row, 8)], blocks.at[g % slots, pl.ds(8 * q, 8)], sem.at[g % slots]
            ).start()

    @pl.when(i == 0)
    def _():
        def some(g, carry):
            start(g)
            return carry

        lax.fori_loop(0, ahead, some, 0)

    @pl.when(i + ahead < pl.num_programs(0))
    def _():
        start(i + ahead)

    slot = i % slots
    pltpu.make_async_copy(blocks.at[slot], blocks.at[slot], sem.at[slot]).wait()
    row = lax.broadcasted_iota(jnp.int32, (size, 8 * size), 0)
    col = lax.broadcasted_iota(jnp.int32, (size, 8 * size), 1)
    want = row * 8 + jnp.concatenate([mods[...]] * (8 * size // 128), axis=1)
    ones = (col == want).astype(F32).astype(BF16)
    out[...] = jnp.dot(ones, blocks[slot], preferred_element_type=F32).astype(BF16)


def pick_rows(emit, tokens):
    (count,) = tokens.shape
    size = 144 if count % 144 == 0 else 64
    ahead = min(2, count // size)
    mods = jnp.broadcast_to((tokens % 8)[:, None], (count, 128))
    return pl.pallas_call(
        functools.partial(pick_kernel, size, ahead),
        out_shape=jax.ShapeDtypeStruct((count, OWN), BF16),
        grid_spec=pltpu.PrefetchScalarGridSpec(
            num_scalar_prefetch=1,
            grid=(count // size,),
            in_specs=[pl.BlockSpec((size, 128), lambda i, tok: (i, 0)), pl.BlockSpec(memory_space=pl.ANY)],
            out_specs=pl.BlockSpec((size, OWN), lambda i, tok: (i, 0)),
            scratch_shapes=[pltpu.VMEM((ahead + 1, 8 * size, OWN), BF16), pltpu.SemaphoreType.DMA((ahead + 1,))],
        ),
        compiler_params=pltpu.CompilerParams(vmem_limit_bytes=60 << 20),
        name="pick",
    )(tokens - tokens % 8, mods, emit)


def run_steps(m, steps, number, t0, trans, emis, state, len_row, log_lik):
    vmem = pl.BlockSpec(memory_space=pltpu.VMEM)
    hbm = pl.BlockSpec(memory_space=pl.ANY)
    depth = 2 if m > 80 else 4
    dma = pltpu.SemaphoreType.DMA
    return pl.pallas_call(
        functools.partial(step_kernel, m, steps, depth),
        out_shape=(jax.ShapeDtypeStruct((SEQS, OWN), F32), jax.ShapeDtypeStruct((1, SEQS), F32)),
        in_specs=[pl.BlockSpec(memory_space=pltpu.SMEM), hbm, hbm, hbm, vmem, vmem],
        out_specs=(hbm, vmem),
        scratch_shapes=[
            pltpu.VMEM((24, PIECE, OWN), BF16),
            pltpu.VMEM((depth, PIECE, OWN), BF16),
            pltpu.VMEM((2, 32, m, PIECE), BF16),
            pltpu.VMEM((m, OWN), BF16),
            pltpu.VMEM((m, OWN), F32),
            pltpu.VMEM((8, m, WIDE), F32),
            pltpu.VMEM((2, N_DEV, 1, 128), F32),
            pltpu.VMEM((128, 128), F32),
            pltpu.VMEM((128, 128), F32),
            pltpu.VMEM((128, 128), F32),
            dma((8,)), dma((depth,)), dma((1,)), dma((1,)), dma((2, 32)), dma((2,)), dma((2,)), dma((2,)), dma((2,)),
        ],
        input_output_aliases={3: 0, 5: 1},
        compiler_params=pltpu.CompilerParams(
            collective_id=number, has_side_effects=True, vmem_limit_bytes=67043328
        ),
        name=f"steps_{m}_{number}",
    )(t0, trans, emis, state, len_row, log_lik)


def solution(mesh):
    def local_run(trans_cols, emit_rows, init_part, token_rows, length_rows):
        emit_t = emit_rows.T

        def emissions(tokens):
            return pick_rows(emit_t, tokens.reshape(-1)).reshape(*tokens.shape, OWN)

        key = length_rows * SEQS + (SEQS - 1 - jnp.arange(SEQS, dtype=jnp.int32))
        rank = jnp.sum((key[None, :] > key[:, None]).astype(jnp.int32), axis=1)
        pick = (rank[None, :] == jnp.arange(SEQS, dtype=jnp.int32)[:, None]).astype(jnp.int32)
        lens = jnp.sum(pick * length_rows[None, :], axis=1)
        tokens = jnp.sum(token_rows.T[:, None, :] * pick[None], axis=2)
        len_row = lens[None, :]

        def segment(m, number, t0, state, log_lik):
            part = lax.dynamic_slice_in_dim(tokens, t0, SEGMENT, axis=0)[:, :m]
            return run_steps(m, SEGMENT, number, jnp.reshape(t0, (1,)), trans_cols, emissions(part), state,
                             len_row, log_lik)

        state, log_lik = run_first(0, init_part[None, :] * emissions(tokens[0]).astype(F32))

        segs = jnp.arange(STEPS // SEGMENT, dtype=jnp.int32)
        live = jnp.sum((lens[None, :] > 1 + SEGMENT * segs[:, None]).astype(jnp.int32), axis=1)
        which = sum((live > m).astype(jnp.int32) for m in ROWS[:-1])
        plan = jnp.sum(which << (3 * segs))

        def later(seg, carried):
            branches = [functools.partial(segment, m, 1 + i) for i, m in enumerate(ROWS)]
            return lax.switch((plan >> (3 * seg)) & 7, branches, 1 + SEGMENT * seg, *carried)

        state, log_lik = lax.fori_loop(0, STEPS // SEGMENT, later, (state, log_lik))
        return jnp.take(log_lik[0], rank, mode="clip"), jnp.take(state, rank, axis=0, mode="clip")

    return jax.shard_map(
        local_run,
        mesh=mesh,
        in_specs=(P(None, "states"), P("states", None), P("states"), P("seqs", None), P("seqs")),
        out_specs=(P("seqs"), P("seqs", "states")),
        check_vma=False,
    )
```

```python
import functools

import jax
import jax.numpy as jnp
from jax import lax
from jax.experimental import pallas as pl
from jax.experimental.pallas import tpu as pltpu
from jax.sharding import PartitionSpec as P

N_DEV = 8
SEQS = 128
OWN = 2048
PIECE = 512
WIDE = 256
STEPS = 63
SEGMENT = 9
ROWS = (32, 48, 64, 80, 96, 112, 128)
REPEATS = {32: 3, 48: 2, 64: 2}
BF16 = jnp.bfloat16
F32 = jnp.float32


def place(g, k):
    late = g // 6
    mid = (g + 6) // 8 - late
    low = 1 - mid - late
    odd = k % 2
    direct = 1 - k // 2
    r = low * g + mid * (2 + 2 * odd + direct) + late * (7 - direct)
    j = low * k + mid * ((g - 2 + 2 * odd) % 4) + late * (g - 6 + 2 * odd)
    return r, j


def distances(me):
    core = me % 2
    xx = (me // 2) % 2
    yy = me // 4

    def dev(r):
        return me + (r % 2) * (1 - 2 * core) + ((r // 2) % 2) * (2 - 4 * xx) + (r // 4) * (4 - 8 * yy)

    return dev


def remote_copy(dev, src, dst, send, recv, r):
    return pltpu.make_async_remote_copy(
        src_ref=src, dst_ref=dst, send_sem=send, recv_sem=recv,
        device_id={"states": dev(r)}, device_id_type=pl.DeviceIdType.MESH,
    )


def signal_all(dev):
    barrier = pltpu.get_barrier_semaphore()
    for r in range(1, N_DEV):
        pl.semaphore_signal(barrier, inc=1, device_id={"states": dev(r)}, device_id_type=pl.DeviceIdType.MESH)
    return barrier


def send_sums(me, dev, sums, part, send, recv):
    part[me] = jnp.sum(sums[...].T, axis=0, keepdims=True)
    for r in range(N_DEV - 1, 0, -1):
        remote_copy(dev, part.at[me], part.at[me], send, recv, r).start()


def add_sums(part, recv):
    pltpu.make_async_copy(part.at[pl.ds(0, 7)], part.at[pl.ds(0, 7)], recv).wait()
    whole = part[0]
    for d in range(1, N_DEV):
        whole = whole + part[d]
    return whole


def first_kernel(raw, alpha, ll, part, sums, send, recv):
    me = lax.axis_index("states")
    dev = distances(me)
    barrier = signal_all(dev)
    both = jnp.zeros((SEQS, 128), F32)
    for q in range(16):
        both = both + raw[:, q * 128:(q + 1) * 128]
    sums[...] = both
    pl.semaphore_wait(barrier, N_DEV - 1)
    send_sums(me, dev, sums, part, send, recv)
    norm = add_sums(part, recv)
    ll[...] = jnp.log(norm)
    scale = jnp.broadcast_to(1.0 / norm, (128, 128)).T
    for q in range(16):
        alpha[:, q * 128:(q + 1) * 128] = raw[:, q * 128:(q + 1) * 128] * scale
    pltpu.make_async_copy(part.at[pl.ds(0, 7)], part.at[pl.ds(0, 7)], send).wait()


def run_first(number, raw):
    vmem = pl.BlockSpec(memory_space=pltpu.VMEM)
    return pl.pallas_call(
        first_kernel,
        out_shape=(jax.ShapeDtypeStruct((SEQS, OWN), F32), jax.ShapeDtypeStruct((1, SEQS), F32)),
        in_specs=[vmem],
        out_specs=(vmem, vmem),
        scratch_shapes=[
            pltpu.VMEM((N_DEV, 1, 128), F32),
            pltpu.VMEM((128, 128), F32),
            pltpu.SemaphoreType.DMA,
            pltpu.SemaphoreType.DMA,
        ],
        compiler_params=pltpu.CompilerParams(collective_id=number, has_side_effects=True, vmem_limit_bytes=8 << 20),
        name="first",
    )(raw)


def step_kernel(m, steps, depth, t0_ref, a_hbm, e_hbm, st_in, len_row, ll_in, st_out, ll_out,
                fixed, ring, gath, e_buf, st, acc, part, sums, recip, len_col,
                fixed_sem, ring_sem, e_sem, st_sem, recv_sem, own_sem, fwd_sem, c_send, c_recv):
    me = lax.axis_index("states")
    dev = distances(me)

    def remote(src, dst, send, recv, r):
        return remote_copy(dev, src, dst, send, recv, r)

    def rows_of(pos):
        r, j = place(pos // 4, pos % 4)
        return a_hbm.at[pl.ds(pl.multiple_of(dev(r) * OWN + j * PIECE, PIECE), PIECE)]

    def begins(b):
        return 4 * b + 2 * ((b + 6) // 8)

    def ring_copy(b):
        return pltpu.make_async_copy(rows_of(begins(b) + 1), ring.at[b % depth], ring_sem.at[b % depth])

    def start_fixed(b, positions):
        for k, pos in enumerate(positions):
            pltpu.make_async_copy(rows_of(pos), fixed.at[3 * b + k], fixed_sem.at[b]).start()

    def start_block(b):
        start_fixed(b, [begins(b), begins(b) + 2, begins(b) + 3])

    def wait_fixed(b):
        pltpu.make_async_copy(fixed.at[pl.ds(3 * b, 3)], fixed.at[pl.ds(3 * b, 3)], fixed_sem.at[b]).wait()

    def send_piece(slot, j, r, pos):
        remote(gath.at[slot, j], gath.at[slot, pos], own_sem.at[slot], recv_sem.at[slot, pos], r).start()

    def send_pair(slot, j):
        send_piece(slot, j, 3, 8 + 4 * j)
        send_piece(slot, j + 2, 5, 9 + 4 * j)
        send_piece(slot, j, 1, 4 + j)
        send_piece(slot, j + 2, 1, 6 + j)

    def send_rest(slot):
        for j in range(2):
            send_piece(slot, j + 2, 3, 16 + 4 * j)
            send_piece(slot, j, 5, 17 + 4 * j)

    def received(slot, pos):
        pltpu.make_async_copy(gath.at[slot, pos], gath.at[slot, pos], recv_sem.at[slot, pos]).wait()

    def forward(slot, pos, to, r):
        remote(gath.at[slot, pos], gath.at[slot, to], fwd_sem.at[slot], recv_sem.at[slot, to], r).start()

    def arrived(slot, g, relay):
        for k in range(2):
            pos = 4 * g + k
            received(slot, pos)

            @pl.when(relay)
            def _():
                forward(slot, pos, pos + 16, 5 - 2 * k)

            forward(slot, pos, pos + 2, 1)

    def product(parts, n):
        cols = slice(n * WIDE, (n + 1) * WIDE)
        got = None
        for left, right in parts:
            rows = left[...]
            if m in REPEATS:
                rows = jnp.concatenate([rows] * REPEATS[m], axis=0)
            one = jnp.dot(rows, right[:, cols], preferred_element_type=F32)
            got = one if got is None else got + one
        return got[:m]

    def next_ring(b):
        ring_copy((b + depth - 1) % 8).start()

    st_copy = pltpu.make_async_copy(st_in.at[pl.ds(0, m)], st, st_sem.at[0])
    st_copy.start()
    ring_copy(0).start()
    start_block(0)
    for b in range(1, depth - 1):
        ring_copy(b).start()
    start_block(1)
    pltpu.make_async_copy(e_hbm.at[0], e_buf, e_sem.at[0]).start()

    barrier = signal_all(dev)
    if m < SEQS:
        sums[...] = jnp.zeros_like(sums)
    t0 = t0_ref[0]
    lens_row = len_row[...]
    len_col[...] = jnp.broadcast_to(lens_row.astype(F32), (128, 128)).T

    def total(slot):
        send_sums(me, dev, sums, part.at[slot], c_send.at[slot], c_recv.at[slot])

    def total_done(slot):
        norm = add_sums(part.at[slot], c_recv.at[slot])
        recip[...] = jnp.broadcast_to(1.0 / norm, (128, 128)).T
        return norm

    def total_sent(slot):
        pltpu.make_async_copy(part.at[slot, pl.ds(0, 7)], part.at[slot, pl.ds(0, 7)], c_send.at[slot]).wait()

    ll_out[...] = ll_in[...]
    st_copy.wait()
    pl.semaphore_wait(barrier, N_DEV - 1)
    for j in range(2):
        for i in (j, j + 2):
            gath[0, i] = st[:, i * PIECE:(i + 1) * PIECE].astype(BF16)
        send_pair(0, j)
    send_rest(0)

    def one_step(s, carry):
        slot = s % 2
        then = 1 - slot

        def block(b, carry):
            @pl.when(b == 1)
            def _():
                for k in range(4):
                    received(slot, 4 + k)

            @pl.when(b == 2)
            def _():
                arrived(slot, 2, True)

                @pl.when(s == 0)
                def _():
                    wait_fixed(7)
                    start_block(3)

                for n in range(8):
                    acc[n] += product([(gath.at[slot, 8], fixed.at[21]), (gath.at[slot, 9], fixed.at[22])], n)

            @pl.when(b >= 2)
            def _():
                arrived(slot, b + 1, b == 2)
                received(slot, 4 * b + 2)
                received(slot, 4 * b + 3)

            next_ring(b)

            @pl.when(s == 0)
            def _():
                wait_fixed(b)

                @pl.when(b == 0)
                def _():
                    start_fixed(7, [8, 9, 30])

                @pl.when(b == 1)
                def _():
                    start_block(2)

                @pl.when((b - 1) * (5 - b) > 0)
                def _():
                    start_block(b + 2)

            ring_copy(b).wait()
            left = [gath.at[slot, begins(b) + k] for k in range(4)]
            right = [fixed.at[3 * b], ring.at[b % depth], fixed.at[3 * b + 1], fixed.at[3 * b + 2]]
            for n in range(8):
                acc[n] = jnp.where(b > 0, acc[n], 0.0) + product(list(zip(left, right)), n)
            return carry

        lax.fori_loop(0, 7, block, 0)

        received(slot, 30)
        received(slot, 31)
        next_ring(7)
        ring_copy(7).wait()
        parts = [(gath.at[slot, 30], fixed.at[23]), (gath.at[slot, 31], ring.at[7 % depth])]
        pltpu.make_async_copy(e_hbm.at[s], e_buf, e_sem.at[0]).wait()
        both = jnp.zeros((m, 128), F32)
        for n in range(8):
            a = (acc[n] + product(parts, n)) * e_buf[:, n * WIDE:(n + 1) * WIDE].astype(F32)
            acc[n] = a
            both = both + (a[:, :128] + a[:, 128:])
        sums[:m] = both

        total(slot)

        @pl.when(s + 1 < steps)
        def _():
            pltpu.make_async_copy(e_hbm.at[s + 1], e_buf, e_sem.at[0]).start()

        pltpu.make_async_copy(gath.at[slot, pl.ds(0, 12)], gath.at[slot, pl.ds(0, 12)], own_sem.at[slot]).wait()
        pltpu.make_async_copy(gath.at[slot, pl.ds(0, 16)], gath.at[slot, pl.ds(0, 16)], fwd_sem.at[slot]).wait()
        norm = total_done(slot)
        t = t0 + s
        ll_out[...] = ll_out[...] + jnp.where(t < lens_row, jnp.log(norm), 0.0)
        total_sent(slot)

        scale = recip[:m]
        live = t.astype(F32) < len_col[:m]
        for j in range(2):
            for i in (j, j + 2):
                for q in range(4):
                    at = i * PIECE + q * 128
                    cols = slice(at, at + 128)
                    new = jnp.where(live, acc[at // WIDE, :, (q % 2) * 128:(q % 2 + 1) * 128] * scale, st[:, cols])
                    st[:, cols] = new
                    gath[then, i, :, q * 128:(q + 1) * 128] = new.astype(BF16)

            @pl.when(s + 1 < steps)
            def _():
                send_pair(then, j)

        @pl.when(s + 1 < steps)
        def _():
            send_rest(then)

        return carry

    lax.fori_loop(0, steps, one_step, 0)

    for b in range(depth - 1):
        ring_copy(b).wait()
    out_copy = pltpu.make_async_copy(st, st_out.at[pl.ds(0, m)], st_sem.at[0])
    out_copy.start()
    out_copy.wait()


def pick_kernel(size, ahead, rows, mods, emit, out, blocks, sem):
    i = pl.program_id(0)
    slots = ahead + 1

    def start(g):
        for q in range(size):
            row = pl.multiple_of(rows[g * size + q], 8)
            pltpu.make_async_copy(
                emit.at[pl.ds(row, 8)], blocks.at[g % slots, pl.ds(8 * q, 8)], sem.at[g % slots]
            ).start()

    @pl.when(i == 0)
    def _():
        def some(g, carry):
            start(g)
            return carry

        lax.fori_loop(0, ahead, some, 0)

    @pl.when(i + ahead < pl.num_programs(0))
    def _():
        start(i + ahead)

    slot = i % slots
    pltpu.make_async_copy(blocks.at[slot], blocks.at[slot], sem.at[slot]).wait()
    row = lax.broadcasted_iota(jnp.int32, (size, 8 * size), 0)
    col = lax.broadcasted_iota(jnp.int32, (size, 8 * size), 1)
    want = row * 8 + jnp.concatenate([mods[...]] * (8 * size // 128), axis=1)
    ones = (col == want).astype(F32).astype(BF16)
    out[...] = jnp.dot(ones, blocks[slot], preferred_element_type=F32).astype(BF16)


def pick_rows(emit, tokens):
    (count,) = tokens.shape
    size = 48 if count % 48 == 0 else 64
    ahead = min(5, count // size)
    mods = jnp.broadcast_to((tokens % 8)[:, None], (count, 128))
    return pl.pallas_call(
        functools.partial(pick_kernel, size, ahead),
        out_shape=jax.ShapeDtypeStruct((count, OWN), BF16),
        grid_spec=pltpu.PrefetchScalarGridSpec(
            num_scalar_prefetch=1,
            grid=(count // size,),
            in_specs=[pl.BlockSpec((size, 128), lambda i, tok: (i, 0)), pl.BlockSpec(memory_space=pl.ANY)],
            out_specs=pl.BlockSpec((size, OWN), lambda i, tok: (i, 0)),
            scratch_shapes=[pltpu.VMEM((ahead + 1, 8 * size, OWN), BF16), pltpu.SemaphoreType.DMA((ahead + 1,))],
        ),
        compiler_params=pltpu.CompilerParams(vmem_limit_bytes=60 << 20),
        name="pick",
    )(tokens - tokens % 8, mods, emit)


def run_steps(m, steps, number, t0, trans, emis, state, len_row, log_lik):
    vmem = pl.BlockSpec(memory_space=pltpu.VMEM)
    hbm = pl.BlockSpec(memory_space=pl.ANY)
    depth = 2 if m > 80 else 4
    dma = pltpu.SemaphoreType.DMA
    return pl.pallas_call(
        functools.partial(step_kernel, m, steps, depth),
        out_shape=(jax.ShapeDtypeStruct((SEQS, OWN), F32), jax.ShapeDtypeStruct((1, SEQS), F32)),
        in_specs=[pl.BlockSpec(memory_space=pltpu.SMEM), hbm, hbm, hbm, vmem, vmem],
        out_specs=(hbm, vmem),
        scratch_shapes=[
            pltpu.VMEM((24, PIECE, OWN), BF16),
            pltpu.VMEM((depth, PIECE, OWN), BF16),
            pltpu.VMEM((2, 32, m, PIECE), BF16),
            pltpu.VMEM((m, OWN), BF16),
            pltpu.VMEM((m, OWN), F32),
            pltpu.VMEM((8, m, WIDE), F32),
            pltpu.VMEM((2, N_DEV, 1, 128), F32),
            pltpu.VMEM((128, 128), F32),
            pltpu.VMEM((128, 128), F32),
            pltpu.VMEM((128, 128), F32),
            dma((8,)), dma((depth,)), dma((1,)), dma((1,)), dma((2, 32)), dma((2,)), dma((2,)), dma((2,)), dma((2,)),
        ],
        input_output_aliases={3: 0, 5: 1},
        compiler_params=pltpu.CompilerParams(
            collective_id=number, has_side_effects=True, vmem_limit_bytes=67043328
        ),
        name=f"steps_{m}_{number}",
    )(t0, trans, emis, state, len_row, log_lik)


def solution(mesh):
    def local_run(trans_cols, emit_rows, init_part, token_rows, length_rows):
        emit_t = emit_rows.T

        def emissions(tokens):
            return pick_rows(emit_t, tokens.reshape(-1)).reshape(*tokens.shape, OWN)

        key = length_rows * SEQS + (SEQS - 1 - jnp.arange(SEQS, dtype=jnp.int32))
        rank = jnp.sum((key[None, :] > key[:, None]).astype(jnp.int32), axis=1)
        pick = (rank[None, :] == jnp.arange(SEQS, dtype=jnp.int32)[:, None]).astype(jnp.int32)
        lens = jnp.sum(pick * length_rows[None, :], axis=1)
        tokens = jnp.sum(token_rows.T[:, None, :] * pick[None], axis=2)
        len_row = lens[None, :]

        def segment(m, number, t0, state, log_lik):
            part = lax.dynamic_slice_in_dim(tokens, t0, SEGMENT, axis=0)[:, :m]
            return run_steps(m, SEGMENT, number, jnp.reshape(t0, (1,)), trans_cols, emissions(part), state,
                             len_row, log_lik)

        state, log_lik = run_first(0, init_part[None, :] * emissions(tokens[0]).astype(F32))

        segs = jnp.arange(STEPS // SEGMENT, dtype=jnp.int32)
        live = jnp.sum((lens[None, :] > 1 + SEGMENT * segs[:, None]).astype(jnp.int32), axis=1)
        which = sum((live > m).astype(jnp.int32) for m in ROWS[:-1])
        plan = jnp.sum(which << (3 * segs))

        def later(seg, carried):
            branches = [functools.partial(segment, m, 1 + i) for i, m in enumerate(ROWS)]
            return lax.switch((plan >> (3 * seg)) & 7, branches, 1 + SEGMENT * seg, *carried)

        state, log_lik = lax.fori_loop(0, STEPS // SEGMENT, later, (state, log_lik))
        return jnp.take(log_lik[0], rank, mode="clip"), jnp.take(state, rank, axis=0, mode="clip")

    return jax.shard_map(
        local_run,
        mesh=mesh,
        in_specs=(P(None, "states"), P("states", None), P("states"), P("seqs", None), P("seqs")),
        out_specs=(P("seqs"), P("seqs", "states")),
        check_vma=False,
    )
```

```python
import functools

import jax
import jax.numpy as jnp
from jax import lax
from jax.experimental import pallas as pl
from jax.experimental.pallas import tpu as pltpu
from jax.sharding import PartitionSpec as P

N_DEV = 8
SEQS = 128
OWN = 2048
PIECE = 512
WIDE = 256
STEPS = 63
SEGMENT = 9
ROWS = (32, 48, 64, 80, 96, 112, 128)
BF16 = jnp.bfloat16
F32 = jnp.float32


def place(g, k):
    late = g // 6
    mid = (g + 6) // 8 - late
    low = 1 - mid - late
    odd = k % 2
    direct = 1 - k // 2
    r = low * g + mid * (2 + 2 * odd + direct) + late * (7 - direct)
    j = low * k + mid * ((g - 2 + 2 * odd) % 4) + late * (g - 6 + 2 * odd)
    return r, j


def distances(me):
    core = me % 2
    xx = (me // 2) % 2
    yy = me // 4

    def dev(r):
        return me + (r % 2) * (1 - 2 * core) + ((r // 2) % 2) * (2 - 4 * xx) + (r // 4) * (4 - 8 * yy)

    return dev


def remote_copy(dev, src, dst, send, recv, r):
    return pltpu.make_async_remote_copy(
        src_ref=src, dst_ref=dst, send_sem=send, recv_sem=recv,
        device_id={"states": dev(r)}, device_id_type=pl.DeviceIdType.MESH,
    )


def signal_all(dev):
    barrier = pltpu.get_barrier_semaphore()
    for r in range(1, N_DEV):
        pl.semaphore_signal(barrier, inc=1, device_id={"states": dev(r)}, device_id_type=pl.DeviceIdType.MESH)
    return barrier


def send_sums(me, dev, sums, part, send, recv):
    part[me] = jnp.sum(sums[...].T, axis=0, keepdims=True)
    for r in range(N_DEV - 1, 0, -1):
        remote_copy(dev, part.at[me], part.at[me], send, recv, r).start()


def add_sums(part, recv):
    pltpu.make_async_copy(part.at[pl.ds(0, 7)], part.at[pl.ds(0, 7)], recv).wait()
    whole = part[0]
    for d in range(1, N_DEV):
        whole = whole + part[d]
    return whole


def first_kernel(raw, alpha, ll, part, sums, send, recv):
    me = lax.axis_index("states")
    dev = distances(me)
    barrier = signal_all(dev)
    both = jnp.zeros((SEQS, 128), F32)
    for q in range(16):
        both = both + raw[:, q * 128:(q + 1) * 128]
    sums[...] = both
    pl.semaphore_wait(barrier, N_DEV - 1)
    send_sums(me, dev, sums, part, send, recv)
    norm = add_sums(part, recv)
    ll[...] = jnp.log(norm)
    scale = jnp.broadcast_to(1.0 / norm, (128, 128)).T
    for q in range(16):
        alpha[:, q * 128:(q + 1) * 128] = raw[:, q * 128:(q + 1) * 128] * scale
    pltpu.make_async_copy(part.at[pl.ds(0, 7)], part.at[pl.ds(0, 7)], send).wait()


def run_first(number, raw):
    vmem = pl.BlockSpec(memory_space=pltpu.VMEM)
    return pl.pallas_call(
        first_kernel,
        out_shape=(jax.ShapeDtypeStruct((SEQS, OWN), F32), jax.ShapeDtypeStruct((1, SEQS), F32)),
        in_specs=[vmem],
        out_specs=(vmem, vmem),
        scratch_shapes=[
            pltpu.VMEM((N_DEV, 1, 128), F32),
            pltpu.VMEM((128, 128), F32),
            pltpu.SemaphoreType.DMA,
            pltpu.SemaphoreType.DMA,
        ],
        compiler_params=pltpu.CompilerParams(collective_id=number, has_side_effects=True, vmem_limit_bytes=8 << 20),
        name="first",
    )(raw)


def step_kernel(m, steps, depth, t0_ref, a_hbm, e_hbm, st_in, len_row, ll_in, st_out, ll_out,
                fixed, ring, gath, e_buf, st, acc, part, sums, recip, len_col,
                fixed_sem, ring_sem, e_sem, st_sem, recv_sem, own_sem, fwd_sem, c_send, c_recv):
    me = lax.axis_index("states")
    dev = distances(me)

    def remote(src, dst, send, recv, r):
        return remote_copy(dev, src, dst, send, recv, r)

    def rows_of(pos):
        r, j = place(pos // 4, pos % 4)
        return a_hbm.at[pl.ds(pl.multiple_of(dev(r) * OWN + j * PIECE, PIECE), PIECE)]

    def begins(b):
        return 4 * b + 2 * ((b + 6) // 8)

    def ring_copy(b):
        return pltpu.make_async_copy(rows_of(begins(b) + 1), ring.at[b % depth], ring_sem.at[b % depth])

    def start_fixed(b, positions):
        for k, pos in enumerate(positions):
            pltpu.make_async_copy(rows_of(pos), fixed.at[3 * b + k], fixed_sem.at[b]).start()

    def start_block(b):
        start_fixed(b, [begins(b), begins(b) + 2, begins(b) + 3])

    def wait_fixed(b):
        pltpu.make_async_copy(fixed.at[pl.ds(3 * b, 3)], fixed.at[pl.ds(3 * b, 3)], fixed_sem.at[b]).wait()

    def send_piece(slot, j, r, pos):
        remote(gath.at[slot, j], gath.at[slot, pos], own_sem.at[slot], recv_sem.at[slot, pos], r).start()

    def send_pair(slot, j):
        send_piece(slot, j, 3, 8 + 4 * j)
        send_piece(slot, j + 2, 5, 9 + 4 * j)
        send_piece(slot, j, 1, 4 + j)
        send_piece(slot, j + 2, 1, 6 + j)

    def send_rest(slot):
        for j in range(2):
            send_piece(slot, j + 2, 3, 16 + 4 * j)
            send_piece(slot, j, 5, 17 + 4 * j)

    def received(slot, pos):
        pltpu.make_async_copy(gath.at[slot, pos], gath.at[slot, pos], recv_sem.at[slot, pos]).wait()

    def forward(slot, pos, to, r):
        remote(gath.at[slot, pos], gath.at[slot, to], fwd_sem.at[slot], recv_sem.at[slot, to], r).start()

    def arrived(slot, g, relay):
        for k in range(2):
            pos = 4 * g + k
            received(slot, pos)

            @pl.when(relay)
            def _():
                forward(slot, pos, pos + 16, 5 - 2 * k)

            forward(slot, pos, pos + 2, 1)

    def product(parts, n):
        cols = slice(n * WIDE, (n + 1) * WIDE)
        got = None
        for left, right in parts:
            rows = left[...]
            if m < SEQS:
                rows = jnp.concatenate([rows] * (SEQS // m) + [rows[:SEQS % m]] * (SEQS % m > 0), axis=0)
            one = jnp.dot(rows, right[:, cols], preferred_element_type=F32)
            got = one if got is None else got + one
        return got[:m]

    def next_ring(b):
        ring_copy((b + depth - 1) % 8).start()

    st_copy = pltpu.make_async_copy(st_in.at[pl.ds(0, m)], st, st_sem.at[0])
    st_copy.start()
    ring_copy(0).start()
    start_block(0)
    for b in range(1, depth - 1):
        ring_copy(b).start()
    start_block(1)
    pltpu.make_async_copy(e_hbm.at[0], e_buf, e_sem.at[0]).start()

    barrier = signal_all(dev)
    if m < SEQS:
        sums[...] = jnp.zeros_like(sums)
    t0 = t0_ref[0]
    lens_row = len_row[...]
    len_col[...] = jnp.broadcast_to(lens_row.astype(F32), (128, 128)).T

    def total(slot):
        send_sums(me, dev, sums, part.at[slot], c_send.at[slot], c_recv.at[slot])

    def total_done(slot):
        norm = add_sums(part.at[slot], c_recv.at[slot])
        recip[...] = jnp.broadcast_to(1.0 / norm, (128, 128)).T
        return norm

    def total_sent(slot):
        pltpu.make_async_copy(part.at[slot, pl.ds(0, 7)], part.at[slot, pl.ds(0, 7)], c_send.at[slot]).wait()

    ll_out[...] = ll_in[...]
    st_copy.wait()
    pl.semaphore_wait(barrier, N_DEV - 1)
    for j in range(2):
        for i in (j, j + 2):
            gath[0, i] = st[:, i * PIECE:(i + 1) * PIECE].astype(BF16)
        send_pair(0, j)
    send_rest(0)

    def one_step(s, carry):
        slot = s % 2
        then = 1 - slot

        def block(b, carry):
            @pl.when(b == 1)
            def _():
                for k in range(4):
                    received(slot, 4 + k)

            @pl.when(b == 2)
            def _():
                arrived(slot, 2, True)

                @pl.when(s == 0)
                def _():
                    wait_fixed(7)
                    start_block(3)

                for n in range(8):
                    acc[n] += product([(gath.at[slot, 8], fixed.at[21]), (gath.at[slot, 9], fixed.at[22])], n)

            @pl.when(b >= 2)
            def _():
                arrived(slot, b + 1, b == 2)
                received(slot, 4 * b + 2)
                received(slot, 4 * b + 3)

            next_ring(b)

            @pl.when(s == 0)
            def _():
                wait_fixed(b)

                @pl.when(b == 0)
                def _():
                    start_fixed(7, [8, 9, 30])

                @pl.when(b == 1)
                def _():
                    start_block(2)

                @pl.when((b - 1) * (5 - b) > 0)
                def _():
                    start_block(b + 2)

            ring_copy(b).wait()
            left = [gath.at[slot, begins(b) + k] for k in range(4)]
            right = [fixed.at[3 * b], ring.at[b % depth], fixed.at[3 * b + 1], fixed.at[3 * b + 2]]
            for n in range(8):
                acc[n] = jnp.where(b > 0, acc[n], 0.0) + product(list(zip(left, right)), n)
            return carry

        lax.fori_loop(0, 7, block, 0)

        received(slot, 30)
        received(slot, 31)
        next_ring(7)
        ring_copy(7).wait()
        parts = [(gath.at[slot, 30], fixed.at[23]), (gath.at[slot, 31], ring.at[7 % depth])]
        pltpu.make_async_copy(e_hbm.at[s], e_buf, e_sem.at[0]).wait()
        both = jnp.zeros((m, 128), F32)
        for n in range(8):
            a = (acc[n] + product(parts, n)) * e_buf[:, n * WIDE:(n + 1) * WIDE].astype(F32)
            acc[n] = a
            both = both + (a[:, :128] + a[:, 128:])
        sums[:m] = both

        total(slot)

        @pl.when(s + 1 < steps)
        def _():
            pltpu.make_async_copy(e_hbm.at[s + 1], e_buf, e_sem.at[0]).start()

        pltpu.make_async_copy(gath.at[slot, pl.ds(0, 12)], gath.at[slot, pl.ds(0, 12)], own_sem.at[slot]).wait()
        pltpu.make_async_copy(gath.at[slot, pl.ds(0, 16)], gath.at[slot, pl.ds(0, 16)], fwd_sem.at[slot]).wait()
        norm = total_done(slot)
        t = t0 + s
        ll_out[...] = ll_out[...] + jnp.where(t < lens_row, jnp.log(norm), 0.0)
        total_sent(slot)

        scale = recip[:m]
        live = t.astype(F32) < len_col[:m]
        for j in range(2):
            for i in (j, j + 2):
                for q in range(4):
                    at = i * PIECE + q * 128
                    cols = slice(at, at + 128)
                    new = jnp.where(live, acc[at // WIDE, :, (q % 2) * 128:(q % 2 + 1) * 128] * scale, st[:, cols])
                    st[:, cols] = new
                    gath[then, i, :, q * 128:(q + 1) * 128] = new.astype(BF16)

            @pl.when(s + 1 < steps)
            def _():
                send_pair(then, j)

        @pl.when(s + 1 < steps)
        def _():
            send_rest(then)

        return carry

    lax.fori_loop(0, steps, one_step, 0)

    for b in range(depth - 1):
        ring_copy(b).wait()
    out_copy = pltpu.make_async_copy(st, st_out.at[pl.ds(0, m)], st_sem.at[0])
    out_copy.start()
    out_copy.wait()


def pick_kernel(size, ahead, rows, mods, emit, out, blocks, sem):
    i = pl.program_id(0)
    slots = ahead + 1

    def start(g):
        for q in range(size):
            row = pl.multiple_of(rows[g * size + q], 2)
            pltpu.make_async_copy(
                emit.at[pl.ds(row, 2)], blocks.at[g % slots, pl.ds(2 * q, 2)], sem.at[g % slots]
            ).start()

    @pl.when(i == 0)
    def _():
        def some(g, carry):
            start(g)
            return carry

        lax.fori_loop(0, ahead, some, 0)

    @pl.when(i + ahead < pl.num_programs(0))
    def _():
        start(i + ahead)

    slot = i % slots
    pltpu.make_async_copy(blocks.at[slot], blocks.at[slot], sem.at[slot]).wait()
    row = lax.broadcasted_iota(jnp.int32, (size, 2 * size), 0)
    col = lax.broadcasted_iota(jnp.int32, (size, 2 * size), 1)
    want = row * 2 + mods[:, :2 * size]
    ones = (col == want).astype(F32).astype(BF16)
    out[...] = jnp.dot(ones, blocks[slot], preferred_element_type=F32).astype(BF16)


def pick_rows(emit, tokens):
    (count,) = tokens.shape
    size = 48 if count % 48 == 0 else 64
    ahead = min(3, count // size)
    mods = jnp.broadcast_to((tokens % 2)[:, None], (count, 128))
    return pl.pallas_call(
        functools.partial(pick_kernel, size, ahead),
        out_shape=jax.ShapeDtypeStruct((count, OWN), BF16),
        grid_spec=pltpu.PrefetchScalarGridSpec(
            num_scalar_prefetch=1,
            grid=(count // size,),
            in_specs=[pl.BlockSpec((size, 128), lambda i, tok: (i, 0)), pl.BlockSpec(memory_space=pl.ANY)],
            out_specs=pl.BlockSpec((size, OWN), lambda i, tok: (i, 0)),
            scratch_shapes=[pltpu.VMEM((ahead + 1, 2 * size, OWN), BF16), pltpu.SemaphoreType.DMA((ahead + 1,))],
        ),
        compiler_params=pltpu.CompilerParams(vmem_limit_bytes=60 << 20),
        name="pick",
    )(tokens - tokens % 2, mods, emit)


def run_steps(m, steps, number, t0, trans, emis, state, len_row, log_lik):
    vmem = pl.BlockSpec(memory_space=pltpu.VMEM)
    hbm = pl.BlockSpec(memory_space=pl.ANY)
    depth = 2 if m > 80 else 4
    dma = pltpu.SemaphoreType.DMA
    return pl.pallas_call(
        functools.partial(step_kernel, m, steps, depth),
        out_shape=(jax.ShapeDtypeStruct((SEQS, OWN), F32), jax.ShapeDtypeStruct((1, SEQS), F32)),
        in_specs=[pl.BlockSpec(memory_space=pltpu.SMEM), hbm, hbm, hbm, vmem, vmem],
        out_specs=(hbm, vmem),
        scratch_shapes=[
            pltpu.VMEM((24, PIECE, OWN), BF16),
            pltpu.VMEM((depth, PIECE, OWN), BF16),
            pltpu.VMEM((2, 32, m, PIECE), BF16),
            pltpu.VMEM((m, OWN), BF16),
            pltpu.VMEM((m, OWN), F32),
            pltpu.VMEM((8, m, WIDE), F32),
            pltpu.VMEM((2, N_DEV, 1, 128), F32),
            pltpu.VMEM((128, 128), F32),
            pltpu.VMEM((128, 128), F32),
            pltpu.VMEM((128, 128), F32),
            dma((8,)), dma((depth,)), dma((1,)), dma((1,)), dma((2, 32)), dma((2,)), dma((2,)), dma((2,)), dma((2,)),
        ],
        input_output_aliases={3: 0, 5: 1},
        compiler_params=pltpu.CompilerParams(
            collective_id=number, has_side_effects=True, vmem_limit_bytes=67043328
        ),
        name=f"steps_{m}_{number}",
    )(t0, trans, emis, state, len_row, log_lik)


def solution(mesh):
    def local_run(trans_cols, emit_rows, init_part, token_rows, length_rows):
        emit_t = emit_rows.T

        def emissions(tokens):
            return pick_rows(emit_t, tokens.reshape(-1)).reshape(*tokens.shape, OWN)

        key = length_rows * SEQS + (SEQS - 1 - jnp.arange(SEQS, dtype=jnp.int32))
        rank = jnp.sum((key[None, :] > key[:, None]).astype(jnp.int32), axis=1)
        pick = (rank[None, :] == jnp.arange(SEQS, dtype=jnp.int32)[:, None]).astype(jnp.int32)
        lens = jnp.sum(pick * length_rows[None, :], axis=1)
        tokens = jnp.sum(token_rows.T[:, None, :] * pick[None], axis=2)
        len_row = lens[None, :]

        def segment(m, number, t0, state, log_lik):
            part = lax.dynamic_slice_in_dim(tokens, t0, SEGMENT, axis=0)[:, :m]
            return run_steps(m, SEGMENT, number, jnp.reshape(t0, (1,)), trans_cols, emissions(part), state,
                             len_row, log_lik)

        state, log_lik = run_first(0, init_part[None, :] * emissions(tokens[0]).astype(F32))

        segs = jnp.arange(STEPS // SEGMENT, dtype=jnp.int32)
        live = jnp.sum((lens[None, :] > 1 + SEGMENT * segs[:, None]).astype(jnp.int32), axis=1)
        which = sum((live > m).astype(jnp.int32) for m in ROWS[:-1])
        plan = jnp.sum(which << (3 * segs))

        def later(seg, carried):
            branches = [functools.partial(segment, m, 1 + i) for i, m in enumerate(ROWS)]
            return lax.switch((plan >> (3 * seg)) & 7, branches, 1 + SEGMENT * seg, *carried)

        state, log_lik = lax.fori_loop(0, STEPS // SEGMENT, later, (state, log_lik))
        return jnp.take(log_lik[0], rank, mode="clip"), jnp.take(state, rank, axis=0, mode="clip")

    return jax.shard_map(
        local_run,
        mesh=mesh,
        in_specs=(P(None, "states"), P("states", None), P("states"), P("seqs", None), P("seqs")),
        out_specs=(P("seqs"), P("seqs", "states")),
        check_vma=False,
    )
```

```python
import functools

import jax
import jax.numpy as jnp
from jax import lax
from jax.experimental import pallas as pl
from jax.experimental.pallas import tpu as pltpu
from jax.sharding import PartitionSpec as P

N_DEV = 8
SEQS = 128
OWN = 2048
PIECE = 512
WIDE = 256
SHORT = 9
SEGMENTS = 7
ROWS = (64, 80, 96, 112, 128)
LONG, LONG_ROWS = 3, 64
BF16 = jnp.bfloat16
F32 = jnp.float32


def place(g, k):
    late = g // 6
    mid = (g + 6) // 8 - late
    low = 1 - mid - late
    odd = k % 2
    direct = 1 - k // 2
    r = low * g + mid * (2 + 2 * odd + direct) + late * (7 - direct)
    j = low * k + mid * ((g - 2 + 2 * odd) % 4) + late * (g - 6 + 2 * odd)
    return r, j


def distances(me):
    core = me % 2
    xx = (me // 2) % 2
    yy = me // 4

    def dev(r):
        return me + (r % 2) * (1 - 2 * core) + ((r // 2) % 2) * (2 - 4 * xx) + (r // 4) * (4 - 8 * yy)

    return dev


def remote_copy(dev, src, dst, send, recv, r):
    return pltpu.make_async_remote_copy(
        src_ref=src, dst_ref=dst, send_sem=send, recv_sem=recv,
        device_id={"states": dev(r)}, device_id_type=pl.DeviceIdType.MESH,
    )


def signal_all(dev):
    barrier = pltpu.get_barrier_semaphore()
    for r in range(1, N_DEV):
        pl.semaphore_signal(barrier, inc=1, device_id={"states": dev(r)}, device_id_type=pl.DeviceIdType.MESH)
    return barrier


def send_sums(me, dev, sums, part, send, recv):
    part[me] = jnp.sum(sums[...].T, axis=0, keepdims=True)
    for r in range(N_DEV - 1, 0, -1):
        remote_copy(dev, part.at[me], part.at[me], send, recv, r).start()


def add_sums(part, recv):
    pltpu.make_async_copy(part.at[pl.ds(0, 7)], part.at[pl.ds(0, 7)], recv).wait()
    whole = part[0]
    for d in range(1, N_DEV):
        whole = whole + part[d]
    return whole


def step_kernel(m, steps, depth, first, t0_ref, a_hbm, e_hbm, st_in, len_row, ll_in, st_out, ll_out,
                fixed, ring, gath, e_buf, st, acc, part, sums, recip, len_col,
                fixed_sem, ring_sem, e_sem, st_sem, recv_sem, own_sem, fwd_sem, c_send, c_recv):
    me = lax.axis_index("states")
    dev = distances(me)

    def remote(src, dst, send, recv, r):
        return remote_copy(dev, src, dst, send, recv, r)

    def rows_of(pos):
        r, j = place(pos // 4, pos % 4)
        return a_hbm.at[pl.ds(pl.multiple_of(dev(r) * OWN + j * PIECE, PIECE), PIECE)]

    def begins(b):
        return 4 * b + 2 * ((b + 6) // 8)

    def ring_copy(b):
        return pltpu.make_async_copy(rows_of(begins(b) + 1), ring.at[b % depth], ring_sem.at[b % depth])

    def start_fixed(b, positions):
        for k, pos in enumerate(positions):
            pltpu.make_async_copy(rows_of(pos), fixed.at[3 * b + k], fixed_sem.at[b]).start()

    def start_block(b):
        start_fixed(b, [begins(b), begins(b) + 2, begins(b) + 3])

    def wait_fixed(b):
        pltpu.make_async_copy(fixed.at[pl.ds(3 * b, 3)], fixed.at[pl.ds(3 * b, 3)], fixed_sem.at[b]).wait()

    def send_piece(slot, j, r, pos):
        remote(gath.at[slot, j], gath.at[slot, pos], own_sem.at[slot], recv_sem.at[slot, pos], r).start()

    def send_pair(slot, j):
        send_piece(slot, j, 3, 8 + 4 * j)
        send_piece(slot, j + 2, 5, 9 + 4 * j)
        send_piece(slot, j, 1, 4 + j)
        send_piece(slot, j + 2, 1, 6 + j)

    def send_rest(slot):
        for j in range(2):
            send_piece(slot, j + 2, 3, 16 + 4 * j)
            send_piece(slot, j, 5, 17 + 4 * j)

    def received(slot, pos):
        pltpu.make_async_copy(gath.at[slot, pos], gath.at[slot, pos], recv_sem.at[slot, pos]).wait()

    def forward(slot, pos, to, r):
        remote(gath.at[slot, pos], gath.at[slot, to], fwd_sem.at[slot], recv_sem.at[slot, to], r).start()

    def arrived(slot, g, relay):
        for k in range(2):
            pos = 4 * g + k
            received(slot, pos)

            @pl.when(relay)
            def _():
                forward(slot, pos, pos + 16, 5 - 2 * k)

            forward(slot, pos, pos + 2, 1)

    def product(parts, n):
        cols = slice(n * WIDE, (n + 1) * WIDE)
        got = None
        for left, right in parts:
            rows = left[...]
            if m < SEQS:
                rows = jnp.concatenate([rows] * (SEQS // m) + [rows[:SEQS % m]] * (SEQS % m > 0), axis=0)
            one = jnp.dot(rows, right[:, cols], preferred_element_type=F32)
            got = one if got is None else got + one
        return got[:m]

    def next_ring(b):
        ring_copy((b + depth - 1) % 8).start()

    st_copy = pltpu.make_async_copy(st_in.at[pl.ds(0, m)], st, st_sem.at[0])
    st_copy.start()
    ring_copy(0).start()
    start_block(0)
    for b in range(1, depth - 1):
        ring_copy(b).start()
    start_block(1)
    pltpu.make_async_copy(e_hbm.at[0], e_buf, e_sem.at[0]).start()

    barrier = signal_all(dev)
    if m < SEQS:
        sums[...] = jnp.zeros_like(sums)
    t0 = t0_ref[0]
    lens_row = len_row[...]
    len_col[...] = jnp.broadcast_to(lens_row.astype(F32), (128, 128)).T

    def total(slot):
        send_sums(me, dev, sums, part.at[slot], c_send.at[slot], c_recv.at[slot])

    def total_done(slot):
        norm = add_sums(part.at[slot], c_recv.at[slot])
        recip[...] = jnp.broadcast_to(1.0 / norm, (128, 128)).T
        return norm

    def total_sent(slot):
        pltpu.make_async_copy(part.at[slot, pl.ds(0, 7)], part.at[slot, pl.ds(0, 7)], c_send.at[slot]).wait()

    st_copy.wait()
    if first:
        both = st[:, :128]
        for q in range(1, 16):
            both = both + st[:, q * 128:(q + 1) * 128]
        sums[...] = both
        pl.semaphore_wait(barrier, N_DEV - 1)
        total(1)
        ll_out[...] = jnp.log(total_done(1))
        total_sent(1)
        for q in range(16):
            st[:, q * 128:(q + 1) * 128] = st[:, q * 128:(q + 1) * 128] * recip[...]
    else:
        ll_out[...] = ll_in[...]
        pl.semaphore_wait(barrier, N_DEV - 1)
    for j in range(2):
        for i in (j, j + 2):
            gath[0, i] = st[:, i * PIECE:(i + 1) * PIECE].astype(BF16)
        send_pair(0, j)
    send_rest(0)

    def one_step(s, carry):
        slot = s % 2
        then = 1 - slot

        def block(b, carry):
            @pl.when(b == 1)
            def _():
                for k in range(4):
                    received(slot, 4 + k)

            @pl.when(b == 2)
            def _():
                arrived(slot, 2, True)

                @pl.when(s == 0)
                def _():
                    wait_fixed(7)
                    start_block(3)

                for n in range(8):
                    acc[n] += product([(gath.at[slot, 8], fixed.at[21]), (gath.at[slot, 9], fixed.at[22])], n)

            @pl.when(b >= 2)
            def _():
                arrived(slot, b + 1, b == 2)
                received(slot, 4 * b + 2)
                received(slot, 4 * b + 3)

            next_ring(b)

            @pl.when(s == 0)
            def _():
                wait_fixed(b)

                @pl.when(b == 0)
                def _():
                    start_fixed(7, [8, 9, 30])

                @pl.when(b == 1)
                def _():
                    start_block(2)

                @pl.when((b - 1) * (5 - b) > 0)
                def _():
                    start_block(b + 2)

            ring_copy(b).wait()
            left = [gath.at[slot, begins(b) + k] for k in range(4)]
            right = [fixed.at[3 * b], ring.at[b % depth], fixed.at[3 * b + 1], fixed.at[3 * b + 2]]
            for n in range(8):
                acc[n] = jnp.where(b > 0, acc[n], 0.0) + product(list(zip(left, right)), n)
            return carry

        lax.fori_loop(0, 7, block, 0)

        received(slot, 30)
        received(slot, 31)
        next_ring(7)
        ring_copy(7).wait()
        parts = [(gath.at[slot, 30], fixed.at[23]), (gath.at[slot, 31], ring.at[7 % depth])]
        pltpu.make_async_copy(e_hbm.at[s], e_buf, e_sem.at[0]).wait()
        both = jnp.zeros((m, 128), F32)
        for n in range(8):
            a = (acc[n] + product(parts, n)) * e_buf[:, n * WIDE:(n + 1) * WIDE].astype(F32)
            acc[n] = a
            both = both + (a[:, :128] + a[:, 128:])
        sums[:m] = both

        total(slot)

        @pl.when(s + 1 < steps)
        def _():
            pltpu.make_async_copy(e_hbm.at[s + 1], e_buf, e_sem.at[0]).start()

        pltpu.make_async_copy(gath.at[slot, pl.ds(0, 12)], gath.at[slot, pl.ds(0, 12)], own_sem.at[slot]).wait()
        pltpu.make_async_copy(gath.at[slot, pl.ds(0, 16)], gath.at[slot, pl.ds(0, 16)], fwd_sem.at[slot]).wait()
        norm = total_done(slot)
        t = t0 + s
        ll_out[...] = ll_out[...] + jnp.where(t < lens_row, jnp.log(norm), 0.0)
        total_sent(slot)

        scale = recip[:m]
        live = t.astype(F32) < len_col[:m]
        for j in range(2):
            for i in (j, j + 2):
                for q in range(4):
                    at = i * PIECE + q * 128
                    cols = slice(at, at + 128)
                    new = jnp.where(live, acc[at // WIDE, :, (q % 2) * 128:(q % 2 + 1) * 128] * scale, st[:, cols])
                    st[:, cols] = new
                    gath[then, i, :, q * 128:(q + 1) * 128] = new.astype(BF16)

            @pl.when(s + 1 < steps)
            def _():
                send_pair(then, j)

        @pl.when(s + 1 < steps)
        def _():
            send_rest(then)

        return carry

    lax.fori_loop(0, steps, one_step, 0)

    for b in range(depth - 1):
        ring_copy(b).wait()
    out_copy = pltpu.make_async_copy(st, st_out.at[pl.ds(0, m)], st_sem.at[0])
    out_copy.start()
    out_copy.wait()


def pick_kernel(size, ahead, tokens, odd, emit, out, blocks, sem):
    i = pl.program_id(0)
    slots = ahead + 1

    def start(g, carry):
        def some(c, carry):
            for k in range(16):
                q = 16 * c + k
                row = pl.multiple_of((tokens[g * size + q] // 2) * 2, 2)
                pltpu.make_async_copy(
                    emit.at[pl.ds(row, 2)], blocks.at[g % slots, pl.ds(pl.multiple_of(2 * q, 2), 2)], sem.at[g % slots]
                ).start()
            return carry

        return lax.fori_loop(0, size // 16, some, carry)

    @pl.when(i == 0)
    def _():
        lax.fori_loop(0, ahead, start, 0)

    @pl.when(i + ahead < pl.num_programs(0))
    def _():
        start(i + ahead, 0)

    slot = i % slots
    pltpu.make_async_copy(blocks.at[slot], blocks.at[slot], sem.at[slot]).wait()
    row = lax.broadcasted_iota(jnp.int32, (size, 2 * size), 0)
    col = lax.broadcasted_iota(jnp.int32, (size, 2 * size), 1)
    want = row * 2 + jnp.concatenate([odd[...]] * 3, axis=1)[:, :2 * size]
    ones = (col == want).astype(F32).astype(BF16)
    out[...] = jnp.dot(ones, blocks[slot], preferred_element_type=F32).astype(BF16)


def pick_rows(emit, tokens):
    (count,) = tokens.shape
    size = 144 if count % 144 == 0 else 64
    ahead = min(2, count // size)
    odd = jnp.broadcast_to((tokens & 1)[:, None], (count, 128))
    return pl.pallas_call(
        functools.partial(pick_kernel, size, ahead),
        out_shape=jax.ShapeDtypeStruct((count, OWN), BF16),
        grid_spec=pltpu.PrefetchScalarGridSpec(
            num_scalar_prefetch=1,
            grid=(count // size,),
            in_specs=[pl.BlockSpec((size, 128), lambda i, tok: (i, 0)), pl.BlockSpec(memory_space=pl.ANY)],
            out_specs=pl.BlockSpec((size, OWN), lambda i, tok: (i, 0)),
            scratch_shapes=[pltpu.VMEM((ahead + 1, 2 * size, OWN), BF16), pltpu.SemaphoreType.DMA((ahead + 1,))],
        ),
        compiler_params=pltpu.CompilerParams(vmem_limit_bytes=60 << 20),
        name="pick",
    )(tokens, odd, emit)


def run_steps(m, steps, first, number, t0, trans, emis, state, len_row, log_lik):
    vmem = pl.BlockSpec(memory_space=pltpu.VMEM)
    hbm = pl.BlockSpec(memory_space=pl.ANY)
    depth = 2 if m > 80 else 4
    dma = pltpu.SemaphoreType.DMA
    return pl.pallas_call(
        functools.partial(step_kernel, m, steps, depth, first),
        out_shape=(jax.ShapeDtypeStruct((SEQS, OWN), F32), jax.ShapeDtypeStruct((1, SEQS), F32)),
        in_specs=[pl.BlockSpec(memory_space=pltpu.SMEM), hbm, hbm, hbm, vmem, vmem],
        out_specs=(hbm, vmem),
        scratch_shapes=[
            pltpu.VMEM((24, PIECE, OWN), BF16),
            pltpu.VMEM((depth, PIECE, OWN), BF16),
            pltpu.VMEM((2, 32, m, PIECE), BF16),
            pltpu.VMEM((m, OWN), BF16),
            pltpu.VMEM((m, OWN), F32),
            pltpu.VMEM((8, m, WIDE), F32),
            pltpu.VMEM((2, N_DEV, 1, 128), F32),
            pltpu.VMEM((128, 128), F32),
            pltpu.VMEM((128, 128), F32),
            pltpu.VMEM((128, 128), F32),
            dma((8,)), dma((depth,)), dma((1,)), dma((1,)), dma((2, 32)), dma((2,)), dma((2,)), dma((2,)), dma((2,)),
        ],
        input_output_aliases={3: 0, 5: 1},
        compiler_params=pltpu.CompilerParams(
            collective_id=number, has_side_effects=True, vmem_limit_bytes=67043328
        ),
        name=f"steps_{m}_{steps}_{number}",
    )(t0, trans, emis, state, len_row, log_lik)


def solution(mesh):
    def local_run(trans_cols, emit_rows, init_part, token_rows, length_rows):
        emit_t = emit_rows.T

        def emissions(tokens):
            return pick_rows(emit_t, tokens.reshape(-1)).reshape(*tokens.shape, OWN)

        key = length_rows * SEQS + (SEQS - 1 - jnp.arange(SEQS, dtype=jnp.int32))
        rank = jnp.sum((key[None, :] > key[:, None]).astype(jnp.int32), axis=1)
        pick = (rank[None, :] == jnp.arange(SEQS, dtype=jnp.int32)[:, None]).astype(jnp.int32)
        lens = jnp.sum(pick * length_rows[None, :], axis=1)
        tokens = jnp.sum(token_rows.T[:, None, :] * pick[None], axis=2)
        len_row = lens[None, :]

        def segment(steps, first, m, number, t0, state, log_lik):
            part = lax.dynamic_slice_in_dim(tokens, t0, steps, axis=0)[:, :m]
            return run_steps(m, steps, first, number, jnp.reshape(t0, (1,)), trans_cols, emissions(part), state,
                             len_row, log_lik)

        state = init_part[None, :] * emissions(tokens[0]).astype(F32)
        state, log_lik = segment(SHORT, True, SEQS, 0, jnp.int32(1), state, jnp.zeros((1, SEQS), F32))

        segs = jnp.arange(1, SEGMENTS, dtype=jnp.int32)
        live = jnp.sum((lens[None, :] > 1 + SHORT * segs[:, None]).astype(jnp.int32), axis=1)
        which = sum((live > m).astype(jnp.int32) for m in ROWS[:-1])
        which = jnp.where((segs == SEGMENTS - LONG) & (live <= LONG_ROWS), len(ROWS), which)
        plan = jnp.sum(which << (3 * segs))

        def later(carried):
            seg, state, log_lik = carried
            kernel = (plan >> (3 * seg)) & 7
            branches = [functools.partial(segment, SHORT, False, m, 1 + i) for i, m in enumerate(ROWS)]
            branches.append(functools.partial(segment, SHORT * LONG, False, LONG_ROWS, 1 + len(ROWS)))
            state, log_lik = lax.switch(kernel, branches, 1 + SHORT * seg, state, log_lik)
            return seg + jnp.where(kernel == len(ROWS), LONG, 1), state, log_lik

        _, state, log_lik = lax.while_loop(lambda carried: carried[0] < SEGMENTS, later, (jnp.int32(1), state, log_lik))
        return jnp.take(log_lik[0], rank, mode="clip"), jnp.take(state, rank, axis=0, mode="clip")

    return jax.shard_map(
        local_run,
        mesh=mesh,
        in_specs=(P(None, "states"), P("states", None), P("states"), P("seqs", None), P("seqs")),
        out_specs=(P("seqs"), P("seqs", "states")),
        check_vma=False,
    )
```
